256 devices in a mesh: lon: 16 (over x_lo, z), lat: 8 (over y, core), ens: 2 (over x_hi).
Axes of the slice: x: 4 (x_hi: 2, x_lo: 2; x = x_hi * 2 + x_lo), y: 4, z: 8, core: 2. Of those that a mesh axis runs over, the one named last changes fastest.
Arguments:
- inputs: bfloat16 [2, 4, 48, 384, 192], P('ens', None, 'lat', 'lon'), may hold values from -6 to 6
- cotangent: bfloat16 [2, 4, 48, 384, 192], P('ens', None, 'lat', 'lon'), may hold values from -6 to 6
- norm1_gain: float32 [192], replicated, may hold values from 0.25 to 1.75
- norm1_offset: float32 [192], replicated, may hold values from -1.5 to 1.5
- qkv_weight: float32 [192, 576], replicated, may hold values from -0.4375 to 0.4375
- qkv_bias: float32 [576], replicated, may hold values from -1.5 to 1.5
- bias_table: float32 [2, 8, 6, 12, 12, 23], P(None, 'lat'), may hold values from -4 to 302
- proj_weight: float32 [192, 192], replicated, may hold values from -0.4375 to 0.4375
- proj_bias: float32 [192], replicated, may hold values from -1.5 to 1.5
- norm2_gain: float32 [192], replicated, may hold values from 0.25 to 1.75
- norm2_offset: float32 [192], replicated, may hold values from -1.5 to 1.5
- fc1_weight: float32 [192, 768], replicated, may hold values from -0.4375 to 0.4375
- fc1_bias: float32 [768], replicated, may hold values from -1.5 to 1.5
- fc2_weight: float32 [768, 192], replicated, may hold values from -0.21875 to 0.21875
- fc2_bias: float32 [192], replicated, may hold values from -1.5 to 1.5
Outputs:
- block_out: bfloat16 [2, 4, 48, 384, 192], P('ens', None, 'lat', 'lon')
- input_grad: bfloat16 [2, 4, 48, 384, 192], P('ens', None, 'lat', 'lon')
- qkv_weight_grad: float32 [192, 576], P(None, 'lon')
- qkv_bias_grad: float32 [576], P('lon')
- proj_weight_grad: float32 [192, 192], P(None, 'lon')
- proj_bias_grad: float32 [192], P('lon')
- fc1_weight_grad: float32 [192, 768], P(None, 'lon')
- fc1_bias_grad: float32 [768], P('lon')
- fc2_weight_grad: float32 [768, 192], P(None, 'lon')
- fc2_bias_grad: float32 [192], P('lon')
- norm1_gain_grad: float32 [192], P('lon')
- norm1_offset_grad: float32 [192], P('lon')
- norm2_gain_grad: float32 [192], P('lon')
- norm2_offset_grad: float32 [192], P('lon')
- bias_table_grad: float32 [2, 8, 6, 12, 12, 23], P(None, 'lat')
The draws below stay inside these ranges and needn't reach their ends.
All inputs are finite; a program needn't handle non-finite values.
Results may differ from the reference program's by a relative error of at most 0.025.
Values may be sent and summed in bfloat16 or wider, within the bound.
No kernel may reach another device: no remote copies, remote signals or barrier semaphores. Data moves between devices by JAX's collectives and lax.ppermute only.
A program may use at most 128 MiB of HBM per device.

```python
import math
import jax
import jax.numpy as jnp
from jax import lax

C = 192
HEADS = 6
FF = 768
WL = 2
WT = 6
WO = 12
LEV = 4
SHIFT = 6
MEMBERS = 2
NLAT = 48
NLON = 384
NWLAT = 8
TOKENS = 147456


def draw_bias_table(key, part):
    table_shape = (LEV // WL, NWLAT, HEADS, WL * WT, WL * WT, 2 * WO - 1)
    return jnp.clip(jax.random.normal(key, table_shape, jnp.float32), -4.0, 4.0)


def block_levels(key, shape, cuts, smallest, top_value):
    def one(axis_at, parts):
        draws = jax.random.uniform(jax.random.fold_in(jax.random.fold_in(key, 6), axis_at), (parts,), jnp.float32, smallest / len(cuts), top_value / len(cuts))
        return jnp.repeat(jnp.exp(draws), shape[axis_at] // parts).reshape((-1,) + (1,) * (len(shape) - axis_at - 1))

    loudness = one(*cuts[0])
    for cut in cuts[1:]:
        loudness = loudness * one(*cut)
    return loudness


def normal_values(own_key, shape, deviation, limit, shards=(), held_as=jnp.bfloat16):
    array = jax.random.normal(own_key, shape, jnp.float32) * deviation
    if len(shards) > 0:
        array = block_levels(own_key, shape, shards, -0.22, 0.18) * array
    return jnp.clip(array, min=-limit, max=limit).astype(held_as)


def setup_inputs(seed: int = 0) -> dict:
    key_list = jax.random.split(jax.random.key(seed), 16)
    return {
        "inputs": normal_values(key_list[0], (MEMBERS, LEV, NLAT, NLON, C), 1.0, 6.0, ((0, 2), (2, 8), (3, 16))),
        "cotangent": normal_values(key_list[1], (MEMBERS, LEV, NLAT, NLON, C), 1.0, 6.0, ((0, 2), (2, 8), (3, 16))),
        "norm1_gain": jnp.clip(1.0 + 0.15 * jax.random.normal(key_list[2], (C,), jnp.float32), 0.25, 1.75),
        "norm1_offset": normal_values(key_list[3], (C,), 0.3, 1.5, (), jnp.float32),
        "qkv_weight": normal_values(key_list[4], (C, 3 * C), C ** -0.5, 0.4375, (), jnp.float32),
        "qkv_bias": normal_values(key_list[5], (3 * C,), 0.3, 1.5, (), jnp.float32),
        "bias_table": draw_bias_table(jax.random.fold_in(key_list[15], 71), 0),
        "proj_weight": normal_values(key_list[7], (C, C), C ** -0.5, 0.4375, (), jnp.float32),
        "proj_bias": normal_values(key_list[8], (C,), 0.3, 1.5, (), jnp.float32),
        "norm2_gain": jnp.clip(1.0 + 0.15 * jax.random.normal(key_list[9], (C,), jnp.float32), 0.25, 1.75),
        "norm2_offset": normal_values(key_list[10], (C,), 0.3, 1.5, (), jnp.float32),
        "fc1_weight": normal_values(key_list[11], (C, FF), C ** -0.5, 0.4375, (), jnp.float32),
        "fc1_bias": normal_values(key_list[12], (FF,), 0.3, 1.5, (), jnp.float32),
        "fc2_weight": normal_values(key_list[13], (FF, C), FF ** -0.5, 0.21875, (), jnp.float32),
        "fc2_bias": normal_values(key_list[14], (C,), 0.3, 1.5, (), jnp.float32),
    }


EPS = 1e-05

def layer_norm(values, gain, offset):
    centre = lax.optimization_barrier(jnp.mean(values, axis=-1, keepdims=True))
    centred = values - centre
    spread = lax.optimization_barrier(jnp.mean(centred * centred, axis=-1, keepdims=True))
    return centred * lax.rsqrt(spread + EPS) * gain + offset

def gelu_tanh(values):
    return jax.nn.gelu(values, approximate=True)

def to_windows(field):
    members, levels, lat_rows, lon_cells, channels = field.shape
    shaped = field.reshape(members, levels // WL, WL, lat_rows // WT, WT, lon_cells // WO, WO, channels)
    shaped = shaped.transpose(0, 1, 3, 5, 2, 4, 6, 7)
    return shaped.reshape(members, levels // WL, lat_rows // WT, lon_cells // WO, WL * WT * WO, channels)

def from_windows(windows):
    members, level_wins, lat_wins, lon_wins, window_size, channels = windows.shape
    shaped = windows.reshape(members, level_wins, lat_wins, lon_wins, WL, WT, WO, channels)
    shaped = shaped.transpose(0, 1, 4, 2, 5, 3, 6, 7)
    return shaped.reshape(members, level_wins * WL, lat_wins * WT, lon_wins * WO, channels)

def offset_picker():
    grid_shape = (WO, WO, 2 * WO - 1)
    lag_index = lax.broadcasted_iota(jnp.int32, grid_shape, 0) - lax.broadcasted_iota(jnp.int32, grid_shape, 1) + (WO - 1)
    return (lag_index == lax.broadcasted_iota(jnp.int32, grid_shape, 2)).astype(jnp.float32)

def expand_bias(table_part, picker):
    level_wins, lat_wins, head_count = table_part.shape[:3]
    expanded = jnp.einsum('vahxyr,ijr->vahxiyj', table_part, picker, precision=lax.Precision.HIGHEST)
    window_size = WL * WT * WO
    return expanded.reshape(level_wins, lat_wins, head_count, window_size, window_size)

def shrink_bias(bias_grad, picker):
    level_wins, lat_wins, head_count = bias_grad.shape[:3]
    shaped = bias_grad.reshape(level_wins, lat_wins, head_count, WL * WT, WO, WL * WT, WO)
    return jnp.einsum('vahxiyj,ijr->vahxyr', shaped, picker, precision=lax.Precision.HIGHEST)

def attend(packed, bias_full, head_count):
    outer = packed.shape[:-1]
    feature_count = packed.shape[-1] // 3
    head_size = feature_count // head_count
    pieces = packed.reshape(outer + (3, head_count, head_size))
    query_rows = pieces[..., 0, :, :]
    key_rows = pieces[..., 1, :, :]
    value_rows = pieces[..., 2, :, :]
    scaling = head_size ** (-0.5)
    scores = jnp.einsum('mvawihd,mvawjhd->mvawhij', query_rows.astype(jnp.float32), key_rows.astype(jnp.float32)) * scaling
    scores = scores + bias_full[None, :, :, None]
    row_peak = lax.optimization_barrier(jnp.max(scores, axis=-1, keepdims=True))
    raised = jnp.exp(scores - row_peak)
    probabilities = raised / lax.optimization_barrier(jnp.sum(raised, axis=-1, keepdims=True))
    weights = probabilities.astype(jnp.bfloat16)
    mixture = jnp.einsum('mvawhij,mvawjhd->mvawihd', weights.astype(jnp.float32), value_rows.astype(jnp.float32)).astype(jnp.bfloat16)
    return (mixture.reshape(outer + (feature_count,)), (query_rows, key_rows, value_rows, probabilities, weights))

def attend_back(mixture_grad, saved_state, head_count):
    query_rows, key_rows, value_rows, probabilities, weights = saved_state
    outer = mixture_grad.shape[:-1]
    feature_count = mixture_grad.shape[-1]
    scaling = (feature_count // head_count) ** (-0.5)
    grad_heads = mixture_grad.reshape(query_rows.shape).astype(jnp.float32)
    prob_grad = jnp.einsum('mvawihd,mvawjhd->mvawhij', grad_heads, value_rows.astype(jnp.float32))
    value_grad = jnp.einsum('mvawhij,mvawihd->mvawjhd', weights.astype(jnp.float32), grad_heads).astype(jnp.bfloat16)
    score_grad = probabilities * (prob_grad - lax.optimization_barrier(jnp.sum(prob_grad * probabilities, axis=-1, keepdims=True)))
    score_low = score_grad.astype(jnp.bfloat16).astype(jnp.float32)
    query_grad = (jnp.einsum('mvawhij,mvawjhd->mvawihd', score_low, key_rows.astype(jnp.float32)) * scaling).astype(jnp.bfloat16)
    key_grad = (jnp.einsum('mvawhij,mvawihd->mvawjhd', score_low, query_rows.astype(jnp.float32)) * scaling).astype(jnp.bfloat16)
    packed_grad = jnp.stack([query_grad, key_grad, value_grad], axis=-3)
    return (packed_grad.reshape(outer + (3 * feature_count,)), score_grad)

def band_pass(inputs, cotangent, table_part, params):
    norm1_gain, norm1_offset, qkv_low, qkv_bias, proj_low, proj_bias, norm2_gain, norm2_offset, fc1_low, fc1_bias, fc2_low, fc2_bias = params
    channels = inputs.shape[-1]
    grid_shape = inputs.shape[:-1]
    inputs_wide = inputs.astype(jnp.float32)
    normed_wide, norm1_back = jax.vjp(layer_norm, inputs_wide, norm1_gain, norm1_offset)
    normed = normed_wide.astype(jnp.bfloat16)
    rolled = jnp.roll(normed, -SHIFT, axis=3)
    packed = jnp.dot(rolled.reshape(-1, channels), qkv_low, preferred_element_type=jnp.float32) + qkv_bias
    packed = to_windows(packed.astype(jnp.bfloat16).reshape(grid_shape + (3 * channels,)))
    picker = offset_picker()
    bias_full = expand_bias(table_part, picker)
    mixture, saved_state = attend(packed, bias_full, HEADS)
    attended = jnp.roll(from_windows(mixture), SHIFT, axis=3).reshape(-1, channels)
    attn_out = (jnp.dot(attended, proj_low, preferred_element_type=jnp.float32) + proj_bias).astype(jnp.bfloat16)
    resid = inputs_wide.reshape(-1, channels) + attn_out.astype(jnp.float32)
    normed2_wide, norm2_back = jax.vjp(layer_norm, resid, norm2_gain, norm2_offset)
    normed2 = normed2_wide.astype(jnp.bfloat16)
    pre_act = jnp.dot(normed2, fc1_low, preferred_element_type=jnp.float32) + fc1_bias
    activ_wide, gelu_back = jax.vjp(gelu_tanh, pre_act)
    activated = activ_wide.astype(jnp.bfloat16)
    block_out = (resid + jnp.dot(activated, fc2_low, preferred_element_type=jnp.float32) + fc2_bias).astype(jnp.bfloat16)
    cot_low = cotangent.reshape(-1, channels)
    cot_wide = cot_low.astype(jnp.float32)
    fc2_bias_grad = lax.optimization_barrier(jnp.sum(cot_wide, axis=0))
    fc2_weight_grad = jnp.dot(activated.T, cot_low, preferred_element_type=jnp.float32)
    act_grad = jnp.dot(cot_low, fc2_low.T, preferred_element_type=jnp.float32)
    pre_grad = gelu_back(act_grad)[0].astype(jnp.bfloat16)
    fc1_bias_grad = lax.optimization_barrier(jnp.sum(pre_grad.astype(jnp.float32), axis=0))
    fc1_weight_grad = jnp.dot(normed2.T, pre_grad, preferred_element_type=jnp.float32)
    normed2_grad = jnp.dot(pre_grad, fc1_low.T, preferred_element_type=jnp.float32)
    resid_part, norm2_gain_grad, norm2_offset_grad = norm2_back(normed2_grad)
    resid_grad = cot_wide + resid_part
    attn_grad = resid_grad.astype(jnp.bfloat16)
    proj_bias_grad = lax.optimization_barrier(jnp.sum(attn_grad.astype(jnp.float32), axis=0))
    proj_weight_grad = jnp.dot(attended.T, attn_grad, preferred_element_type=jnp.float32)
    attended_grad = jnp.dot(attn_grad, proj_low.T, preferred_element_type=jnp.float32).astype(jnp.bfloat16)
    rolled_grad = jnp.roll(attended_grad.reshape(grid_shape + (channels,)), -SHIFT, axis=3)
    packed_grad, score_grad = attend_back(to_windows(rolled_grad), saved_state, HEADS)
    table_grad = shrink_bias(lax.optimization_barrier(jnp.sum(score_grad, axis=(0, 3))), picker)
    qkv_grad = jnp.roll(from_windows(packed_grad), SHIFT, axis=3).reshape(-1, 3 * channels)
    qkv_bias_grad = lax.optimization_barrier(jnp.sum(qkv_grad.astype(jnp.float32), axis=0))
    qkv_weight_grad = jnp.dot(normed.reshape(-1, channels).T, qkv_grad, preferred_element_type=jnp.float32)
    normed_grad = jnp.dot(qkv_grad, qkv_low.T, preferred_element_type=jnp.float32)
    input_part, norm1_gain_grad, norm1_offset_grad = norm1_back(normed_grad.reshape(grid_shape + (channels,)))
    input_grad = (resid_grad.reshape(grid_shape + (channels,)) + input_part).astype(jnp.bfloat16)
    grads = (qkv_weight_grad, qkv_bias_grad, proj_weight_grad, proj_bias_grad, fc1_weight_grad, fc1_bias_grad, fc2_weight_grad, fc2_bias_grad, norm1_gain_grad, norm1_offset_grad, norm2_gain_grad, norm2_offset_grad)
    return (block_out.reshape(grid_shape + (channels,)), input_grad, grads, table_grad)

def reference(inputs, cotangent, norm1_gain, norm1_offset, qkv_weight, qkv_bias, bias_table, proj_weight, proj_bias, norm2_gain, norm2_offset, fc1_weight, fc1_bias, fc2_weight, fc2_bias):
    band_count = NLAT // WT
    params = (norm1_gain, norm1_offset, qkv_weight.astype(jnp.bfloat16), qkv_bias, proj_weight.astype(jnp.bfloat16), proj_bias, norm2_gain, norm2_offset, fc1_weight.astype(jnp.bfloat16), fc1_bias, fc2_weight.astype(jnp.bfloat16), fc2_bias)

    def to_bands(field):
        shaped = field.reshape(MEMBERS, LEV, band_count, WT, NLON, field.shape[-1])
        return jnp.moveaxis(shaped, 2, 0)

    def from_bands(stacked):
        return jnp.moveaxis(stacked, 0, 2).reshape(MEMBERS, LEV, NLAT, NLON, stacked.shape[-1])
    tables = jnp.moveaxis(bias_table, 1, 0)
    shapes = (qkv_weight, qkv_bias, proj_weight, proj_bias, fc1_weight, fc1_bias, fc2_weight, fc2_bias, norm1_gain, norm1_offset, norm2_gain, norm2_offset)
    initial = tuple((jnp.zeros(entry.shape, jnp.float32) for entry in shapes))

    def advance(carried, slices):
        inputs_band, cot_band, table_band = slices
        block_band, grad_band, grads, table_grad = band_pass(inputs_band, cot_band, table_band[:, None], params)
        summed = tuple((left + right for left, right in zip(carried, grads)))
        return (summed, (block_band, grad_band, table_grad[:, 0]))
    totals, (blocks, input_grads, table_grads) = lax.scan(advance, initial, (to_bands(inputs), to_bands(cotangent), tables))
    factor = 1.0 / math.sqrt(TOKENS)
    scaled = tuple((factor * entry for entry in totals))
    return (from_bands(blocks), from_bands(input_grads), scaled[0], scaled[1], scaled[2], scaled[3], scaled[4], scaled[5], scaled[6], scaled[7], scaled[8], scaled[9], scaled[10], scaled[11], jnp.moveaxis(table_grads, 0, 1))
```

```python
import math

import jax
import jax.numpy as jnp
import numpy as np
from jax import lax
from jax.experimental import pallas as pl
from jax.experimental.pallas import tpu as pltpu
from jax.sharding import Mesh
from jax.sharding import PartitionSpec as P

C = 192
HEADS = 6
FF = 768
WO = 12
ROWS = 144
LANES = 896
HX = 72
TAB = 384
EPS = 1e-05
SCALE = 32 ** -0.5
F32 = jnp.float32
BF16 = jnp.bfloat16
FACTOR = 1.0 / math.sqrt(147456)
GELU_A = 0.044715
GELU_C = math.sqrt(2.0 / math.pi)
PART = 128
SLOT = 32


def nn(a, b):
    return lax.dot_general(a, b, (((1,), (0,)), ((), ())), preferred_element_type=F32)


def nt(a, b):
    return lax.dot_general(a, b, (((1,), (1,)), ((), ())), preferred_element_type=F32)


def tn(a, b):
    return lax.dot_general(a, b, (((0,), (0,)), ((), ())), preferred_element_type=F32)


def token_spread():
    out = np.zeros((ROWS, LANES), np.float32)
    for i in range(WO):
        for h in range(HEADS):
            for x in range(WO):
                out[12 * x + i, HX * i + 12 * h + x] = 1.0
    return out


def head_mask():
    out = np.zeros((C, LANES), np.float32)
    for lane in range(12 * HX):
        h = (lane % HX) // 12
        out[32 * h : 32 * h + 32, lane] = 1.0
    return out


def lag_select():
    out = np.zeros((12 * ROWS, TAB), np.float32)
    for i in range(12):
        for y in range(12):
            for j in range(12):
                out[i * ROWS + 12 * y + j, 32 * y + i - j + 11] = 1.0
    return out


def bias_places():
    rows_a = np.zeros((16, 1344), np.float32)
    cols_a = np.zeros((1344, 128), np.float32)
    rows_b = np.zeros((16, 1152), np.float32)
    cols_b = np.zeros((1152, 128), np.float32)
    for n in range(576):
        rows_a[n // 36, n] = 1.0
        cols_a[n, n % 36] = 1.0
    for n in range(768):
        rows_a[n // 48, 576 + n] = 1.0
        cols_a[576 + n, 36 + n % 48] = 1.0
    for k in range(6):
        for n in range(192):
            rows_b[n // 12, 192 * k + n] = 1.0
            cols_b[192 * k + n, 12 * k + n % 12] = 1.0
    return rows_a, cols_a, rows_b, cols_b


def prep_kernel(qkv_ref, proj_ref, fc1_ref, fc2_ref, tab_ref, sel_ref,
                wt_ref, projb_ref, fc1b_ref, fc2b_ref, bias_ref):
    wt_ref[...] = qkv_ref[...].T.astype(BF16)
    projb_ref[...] = proj_ref[...].astype(BF16)
    fc1b_ref[...] = fc1_ref[...].astype(BF16)
    fc2b_ref[...] = fc2_ref[...].astype(BF16)
    tiles = []
    for t in range(3):
        tile = None
        for k in range(4):
            piece = tab_ref[pl.ds(4 * t + k, ROWS, stride=12), :]
            piece = jnp.concatenate([piece, jnp.zeros((ROWS, 105), F32)], axis=1)
            if k:
                piece = pltpu.roll(piece, 32 * k, 1)
            tile = piece if tile is None else tile + piece
        tiles.append(tile)
    table = jnp.concatenate(tiles, axis=1)
    high = table.astype(BF16)
    low = (table - high.astype(F32)).astype(BF16)
    pieces = [[], []]
    for i in range(12):
        sel = sel_ref[ROWS * i : ROWS * i + ROWS, :]
        got = nt(sel, high) + nt(sel, low)
        pieces[0].append(got[:, :HX])
        pieces[1].append(got[:, HX:])
    for v in range(2):
        spare = jnp.zeros((ROWS, LANES - 12 * HX), F32)
        bias_ref[v] = jnp.concatenate(pieces[v] + [spare], axis=1)


def column(row):
    size = row.shape[1]
    eye = lax.broadcasted_iota(jnp.int32, (size, size), 0) == lax.broadcasted_iota(
        jnp.int32, (size, size), 1
    )
    return jnp.sum(jnp.where(eye, row, 0.0), axis=1, keepdims=True)


def window_picks():
    r = lax.broadcasted_iota(jnp.int32, (576, 128), 0).astype(F32)
    m = jnp.floor((r + 0.5) * (1.0 / 12.0))
    j = r - 12.0 * m
    second = m >= 24.0
    n = jnp.where(second, m - 24.0, m)
    src = jnp.where(second, 24.0 * n + 18.0 + j, 24.0 * n + 6.0 + j)
    src = jnp.where(second & (j >= 6.0), 570.0 + 8.0 * n + j, src)
    lane = lax.broadcasted_iota(jnp.int32, (576, 128), 1).astype(F32)
    tiles = [jnp.where(src == lane + 128.0 * t, 1.0, 0.0).astype(BF16) for t in range(6)]
    return jnp.concatenate(tiles, axis=1)


def natural_picks():
    p = lax.broadcasted_iota(jnp.int32, (768, 128), 0).astype(F32)
    own = p < 576.0
    q = p - 576.0
    n = jnp.where(own, jnp.floor((p + 0.5) * (1.0 / 24.0)), jnp.floor((q + 0.5) * 0.125))
    c = jnp.where(own, p - 24.0 * n, q - 8.0 * n)
    inner = jnp.where(c < 18.0, 12.0 * n + c - 6.0, 288.0 + 12.0 * n + c - 18.0)
    inner = jnp.where(c < 6.0, -1.0, inner)
    outer = jnp.where(c < 6.0, 294.0 + 12.0 * n + c, -1.0)
    dst = jnp.where(own, inner, outer)
    lane = lax.broadcasted_iota(jnp.int32, (768, 128), 1).astype(F32)
    tiles = [jnp.where(dst == lane + 128.0 * t, 1.0, 0.0).astype(BF16) for t in range(5)]
    return jnp.concatenate(tiles, axis=1)[:, :576]


def norm_parts(values):
    centre = jnp.sum(values, axis=1, keepdims=True) * (1.0 / C)
    centred = values - centre
    spread = jnp.sum(centred * centred, axis=1, keepdims=True) * (1.0 / C)
    inverse = lax.rsqrt(spread + EPS)
    return centred * inverse, inverse


def norm_back(grad, hat, inverse, gain):
    scaled = grad * gain
    first = jnp.sum(scaled, axis=1, keepdims=True) * (1.0 / C)
    second = jnp.sum(scaled * hat, axis=1, keepdims=True) * (1.0 / C)
    return inverse * (scaled - first - hat * second)


def main_kernel(core_ref, x_ref, cot_ref, n1g_ref, n1o_ref, qb_ref, pb_ref, n2g_ref, n2o_ref,
                f1b_ref, f2b_ref, spread_ref, mask_ref, sel_ref, ra_ref, ca_ref, rb_ref, cb_ref,
                halo_ref, bias_ref, wt_ref, proj_ref, fc1_ref, fc2_ref,
                both_ref, edge_ref, own_ref, send_ref, low_ref, sum_ref, stage_ref, tab_ref):
    n1g, n1o, qb, pb, n2g, n2o, f1b, f2b = (
        ref[...].reshape(1, -1)
        for ref in (n1g_ref, n1o_ref, qb_ref, pb_ref, n2g_ref, n2o_ref, f1b_ref, f2b_ref)
    )
    picks = window_picks()
    xw = nn(picks, jnp.concatenate([x_ref[...], halo_ref[0]], axis=0))
    cw = nn(picks, jnp.concatenate([cot_ref[...], halo_ref[1]], axis=0))
    cot_low = cw.astype(BF16)
    hat1, inv1 = norm_parts(xw)
    normed = (hat1 * n1g + n1o).astype(BF16)
    wq = wt_ref[0:192, :]
    wk = wt_ref[192:384, :]
    wv = wt_ref[384:576, :]
    bq_row = qb[:, 0:192]
    bk_row = qb[:, 192:384]
    bv_row = qb[:, 384:576]
    bq = column(bq_row)
    bk = column(bk_row)
    bv = column(bv_row)
    keys = (nt(normed, wk) + bk_row).astype(BF16)
    values = (nt(normed, wv) + bv_row).astype(BF16)
    spread = spread_ref[...]
    mask = mask_ref[...]
    saved = []
    attended = []
    for g in range(4):
        rows = slice(ROWS * g, ROWS * g + ROWS)
        own = normed[rows]
        query_t = (nt(wq, own) + bq).astype(BF16)
        value_t = (nt(wv, own) + bv).astype(BF16)
        query_bd = nn(query_t, spread).astype(BF16) * mask
        scores = nn(keys[rows], query_bd) * SCALE + bias_ref[g % 2]
        peak = jnp.max(scores, axis=0, keepdims=True)
        raised = jnp.exp(scores - peak)
        total = jnp.sum(raised, axis=0, keepdims=True)
        weights = (raised * (1.0 / total)).astype(BF16)
        mixed = nn(value_t, weights).astype(BF16) * mask
        attended.append(nt(spread, mixed).astype(BF16))
        saved.append((query_bd, weights))
    attended = jnp.concatenate(attended, axis=0)
    attn_out = (nn(attended, proj_ref[...]) + pb).astype(BF16)
    resid = xw + attn_out.astype(F32)
    hat2, inv2 = norm_parts(resid)
    normed2 = (hat2 * n2g + n2o).astype(BF16)
    acts = []
    grads = []
    f1_sums = []
    for g in range(4):
        rows = slice(ROWS * g, ROWS * g + ROWS)
        u = nn(normed2[rows], fc1_ref[...]) + f1b
        square = u * u
        t = jnp.tanh(GELU_C * (u + GELU_A * (square * u)))
        half = 0.5 * (1.0 + t)
        acts.append((u * half).astype(BF16))
        slope = half + 0.5 * u * (1.0 - t * t) * (GELU_C + (3.0 * GELU_A * GELU_C) * square)
        act_grad = nn(cot_low[rows], fc2_ref[...])
        pre = (act_grad * slope).astype(BF16)
        grads.append(pre)
        f1_sums.append(jnp.sum(pre.astype(F32), axis=0, keepdims=True))
    activated = jnp.concatenate(acts, axis=0)
    pre_grad = jnp.concatenate(grads, axis=0)
    f1_sum = f1_sums[0] + f1_sums[1] + f1_sums[2] + f1_sums[3]
    block = (resid + nt(activated, fc2_ref[...]) + f2b).astype(BF16)
    back = natural_picks()
    placed = nn(back, block).astype(BF16)
    both_ref[0] = placed[:576]
    edge_ref[0] = placed[576:]
    n2_grad = nt(pre_grad, fc1_ref[...])
    n2g_sum = jnp.sum(n2_grad * hat2, axis=0, keepdims=True)
    n2o_sum = jnp.sum(n2_grad, axis=0, keepdims=True)
    resid_grad = cw + norm_back(n2_grad, hat2, inv2, n2g)
    attn_grad = resid_grad.astype(BF16)
    pb_sum = jnp.sum(attn_grad.astype(F32), axis=0, keepdims=True)
    f2_sum = jnp.sum(cw, axis=0, keepdims=True)
    grad_q = []
    grad_k = []
    grad_v = []
    for g in range(4):
        rows = slice(ROWS * g, ROWS * g + ROWS)
        query_bd, weights = saved[g]
        own = normed[rows]
        grad_t = nt(proj_ref[...], attn_grad[rows]).astype(BF16)
        grad_bd = nn(grad_t, spread).astype(BF16) * mask
        prob_grad = nn(values[rows], grad_bd)
        probs = weights.astype(F32)
        shared = jnp.sum(probs * prob_grad, axis=0, keepdims=True)
        score_grad = probs * (prob_grad - shared)
        if g < 2:
            sum_ref[g] = score_grad
        else:
            sum_ref[g - 2] += score_grad
        low = score_grad.astype(BF16)
        grad_v.append(nt(weights, grad_bd).astype(BF16))
        grad_k.append((nt(low, query_bd) * SCALE).astype(BF16))
        key_t = (nt(wk, own) + bk).astype(BF16)
        mixed = (nn(key_t, low) * SCALE).astype(BF16) * mask
        grad_q.append(nt(spread, mixed).astype(BF16))
    dq = jnp.concatenate(grad_q, axis=0)
    dk = jnp.concatenate(grad_k, axis=0)
    dv = jnp.concatenate(grad_v, axis=0)
    n1_grad = nn(dq, wq) + nn(dk, wk) + nn(dv, wv)
    n1g_sum = jnp.sum(n1_grad * hat1, axis=0, keepdims=True)
    n1o_sum = jnp.sum(n1_grad, axis=0, keepdims=True)
    input_grad = (resid_grad + norm_back(n1_grad, hat1, inv1, n1g)).astype(BF16)
    placed = nn(back, input_grad).astype(BF16)
    both_ref[1] = placed[:576]
    edge_ref[1] = placed[576:]
    sums = [jnp.sum(d.astype(F32), axis=0, keepdims=True) for d in (dq, dk, dv)]
    for v in range(2):
        turned = sum_ref[v].T
        total = jnp.zeros((HX, TAB), F32)
        for i in range(12):
            piece = turned[HX * i : HX * i + HX, :].astype(BF16)
            total = total + nn(piece, sel_ref[ROWS * i : ROWS * i + ROWS, :])
        for t in range(3):
            tab_ref[ROWS * t + HX * v : ROWS * t + HX * v + HX, :] = total[:, 128 * t : 128 * t + 128]
    tab_ref[3 * ROWS :, :] = jnp.zeros((16 * SLOT - 3 * ROWS, 128), F32)
    low_ref[...] = tab_ref[...].astype(BF16)
    dw_q = tn(dq, normed)
    dw_k = tn(dk, normed)
    dw_v = tn(dv, normed)
    dw_qkv = jnp.concatenate([dw_q, dw_k, dw_v], axis=0)
    dw_p = tn(attn_grad, attended)
    dw_1 = tn(pre_grad, normed2)
    dw_2 = tn(cot_low, activated)
    vec_a = jnp.concatenate(sums + [f1_sum[:, 0:192], f1_sum[:, 192:384], f1_sum[:, 384:576], f1_sum[:, 576:768]], axis=1)
    vec_b = jnp.concatenate([pb_sum, f2_sum, n1g_sum, n1o_sum, n2g_sum, n2o_sum], axis=1)
    row_a = nn((ra_ref[...].astype(F32) * vec_a).astype(BF16), ca_ref[...])
    row_b = nn((rb_ref[...].astype(F32) * vec_b).astype(BF16), cb_ref[...])
    for l in range(16):
        a36 = dw_qkv[36 * l : 36 * l + 36]
        a12 = dw_p[12 * l : 12 * l + 12]
        b48 = dw_1[48 * l : 48 * l + 48]
        d12 = dw_2[12 * l : 12 * l + 12]
        top = PART * l
        stage_ref[0, top : top + 36, :] = a36[:, :128]
        stage_ref[0, top + 36 : top + 48, :] = a12[:, :128]
        a_rest = jnp.concatenate([a36[:, 128:], a12[:, 128:]], axis=0)
        stage_ref[0, top + 48 : top + 96, :] = jnp.concatenate([a_rest, b48[:, 128:]], axis=1)
        stage_ref[0, top + 96 : top + 108, :] = d12[:, 640:]
        stage_ref[0, top + 108 : top + 112, :] = jnp.zeros((4, 128), F32)
        stage_ref[0, top + 112 : top + 128, :] = jnp.concatenate(
            [row_a[l : l + 1], row_b[l : l + 1], jnp.zeros((14, 128), F32)], axis=0
        )
        stage_ref[1, top : top + 48, :] = b48[:, :128]
        for b in range(5):
            piece = d12[:, 128 * b : 128 * b + 128]
            stage_ref[1, top + 48 + 16 * b : top + 64 + 16 * b, :] = jnp.concatenate(
                [piece, jnp.zeros((4, 128), F32)], axis=0
            )
    core = core_ref[0]
    for k in range(8):
        for l in range(16):
            rows = slice(PART * l + 16 * k, PART * l + 16 * k + 16)
            spot = slice(16 * l, 16 * l + 16)
            own_ref[k, spot, :] = stage_ref[core, rows, :].astype(BF16)
            send_ref[k, spot, :] = stage_ref[1 - core, rows, :].astype(BF16)


def join_kernel(own_ref, got_ref, out_ref):
    out_ref[...] = (own_ref[...].astype(F32) + got_ref[...].astype(F32)).astype(BF16)


def band_sum_kernel(in_ref, tab_ref, twin_ref, out_ref):
    total = in_ref[0].astype(F32)
    for k in range(1, 8):
        total = total + in_ref[k].astype(F32)
    low = total.astype(BF16)
    table = (tab_ref[...].astype(F32) + twin_ref[...].astype(F32)).astype(BF16)
    for l in range(16):
        out_ref[l, 0:16, :] = low[16 * l : 16 * l + 16]
        out_ref[l, 16:, :] = table[SLOT * l : SLOT * l + SLOT]


def lon_sum_kernel(in_ref, part_ref, tab_ref):
    total = in_ref[0].astype(F32)
    for l in range(1, 16):
        total = total + in_ref[l].astype(F32)
    low = total.astype(BF16)
    for k in range(16):
        part_ref[k] = low[:16]
        tab_ref[k] = low[16:]


def final_kernel(part_ref, tab_ref, qw_ref, pw_ref, f1_ref, f2_ref, qb_ref, pb_ref, f1b_ref, f2b_ref,
                 n1g_ref, n1o_ref, n2g_ref, n2o_ref, out_tab_ref):
    def half(core):
        rows = [part_ref[4 * y + 2 * core + e] for y in range(4) for e in range(2)]
        return jnp.concatenate(rows, axis=0).astype(F32) * FACTOR

    first = half(0)
    second = half(1)
    a = jnp.concatenate([first[0:48], first[48:96, 0:64]], axis=1)
    qw_ref[...] = a[0:36]
    pw_ref[...] = a[36:48]
    f1_ref[...] = jnp.concatenate([second[0:48], first[48:96, 64:128]], axis=1)
    d = [second[48 + 16 * k : 60 + 16 * k] for k in range(5)] + [first[96:108]]
    f2_ref[...] = jnp.concatenate(d, axis=1)
    va = first[112:113]
    vb = first[113:114]
    qb_ref[...] = va[:, 0:36].reshape(36)
    f1b_ref[...] = va[:, 36:84].reshape(48)
    for k, ref in enumerate((pb_ref, f2b_ref, n1g_ref, n1o_ref, n2g_ref, n2o_ref)):
        ref[...] = vb[:, 12 * k : 12 * k + 12].reshape(12)
    tab = tab_ref[...].astype(F32)
    for t in range(3):
        tile = tab[ROWS * t : ROWS * t + ROWS]
        for k in range(4):
            piece = pltpu.roll(tile, 128 - 32 * k, 1) if k else tile
            out_tab_ref[pl.ds(4 * t + k, ROWS, stride=12), :] = piece[:, :23]


def call(kernel, out_shape, smem=0, far=0, near=0, limit=8, scratch=()):
    count = smem + far + near
    specs = [pl.BlockSpec(memory_space=pltpu.SMEM)] * smem + [
        pl.BlockSpec(memory_space=pltpu.VMEM)
    ] * (far + near)
    run = pl.pallas_call(
        kernel,
        out_shape=out_shape,
        in_specs=specs,
        out_specs=jax.tree.map(lambda _: pl.BlockSpec(memory_space=pltpu.VMEM), out_shape),
        scratch_shapes=scratch,
        compiler_params=pltpu.CompilerParams(vmem_limit_bytes=limit << 20),
    )

    def go(*args):
        kept = args[: smem + far] + tuple(
            pltpu.with_memory_space_constraint(a, pltpu.VMEM) for a in args[smem + far :]
        )
        assert len(args) == count
        return run(*kept)

    return go


def near(dims, dtype):
    return pltpu.VMEM(dims, dtype)


def shape(dims, dtype):
    return jax.ShapeDtypeStruct(dims, dtype)


def on_device(inputs, cotangent, norm1_gain, norm1_offset, qkv_weight, qkv_bias, bias_table,
              proj_weight, proj_bias, norm2_gain, norm2_offset, fc1_weight, fc1_bias,
              fc2_weight, fc2_bias):
    grid = inputs.shape
    x = inputs.reshape(576, C)
    cot = cotangent.reshape(576, C)
    edge = jnp.stack([inputs[0, :, :, :8, :].reshape(192, C), cotangent[0, :, :, :8, :].reshape(192, C)])
    halo = lax.ppermute(edge, "lon", [(k, (k - 1) % 16) for k in range(16)])
    spread = jnp.asarray(token_spread(), BF16)
    mask = jnp.asarray(head_mask(), BF16)
    sel = jnp.asarray(lag_select(), BF16)
    ra, ca, rb, cb = (jnp.asarray(a, BF16) for a in bias_places())
    table = bias_table.reshape(12 * ROWS, 23)
    wt, proj, fc1, fc2, bias = call(
        prep_kernel,
        [near((576, C), BF16), near((C, C), BF16), near((C, FF), BF16), near((C, FF), BF16),
         near((2, ROWS, LANES), F32)],
        far=6,
        limit=16,
    )(qkv_weight, proj_weight, fc1_weight, fc2_weight.T, table, sel)
    core = lax.axis_index("core").astype(jnp.int32).reshape(1)
    both, ends, own, send, tab = call(
        main_kernel,
        [shape((2, 576, C), BF16), near((2, 192, C), BF16), near((8, 256, 128), BF16),
         near((8, 256, 128), BF16), near((16 * SLOT, 128), BF16)],
        smem=1,
        far=17,
        near=6,
        limit=36,
        scratch=[pltpu.VMEM((2, ROWS, LANES), F32), pltpu.VMEM((2, 16 * PART, 128), F32),
                 pltpu.VMEM((16 * SLOT, 128), F32)],
    )(core, x, cot, norm1_gain, norm1_offset, qkv_bias, proj_bias,
      norm2_gain, norm2_offset, fc1_bias, fc2_bias, spread, mask, sel, ra, ca, rb, cb,
      halo, bias, wt, proj, fc1, fc2)
    got = lax.ppermute(send, "core", [(0, 1), (1, 0)])
    twin = lax.ppermute(tab, "ens", [(0, 1), (1, 0)])
    home = lax.ppermute(ends, "lon", [(k, (k + 1) % 16) for k in range(16)])
    joined = call(join_kernel, near((8, 256, 128), BF16), near=2)(own, got)
    bands = lax.all_to_all(joined, ("y", "ens"), split_axis=0, concat_axis=0, tiled=True)
    merged = call(band_sum_kernel, near((16, 16 + SLOT, 128), BF16), near=3)(bands, tab, twin)
    arrived = lax.all_to_all(merged, "lon", split_axis=0, concat_axis=0, tiled=True)
    part, tab_copies = call(
        lon_sum_kernel, [near((16, 16, 128), BF16), near((16, SLOT, 128), BF16)], near=1
    )(arrived)
    parts = lax.all_to_all(part, ("y", "core", "ens"), split_axis=0, concat_axis=0, tiled=True)
    tab_all = lax.all_to_all(tab_copies, "lon", split_axis=0, concat_axis=0, tiled=True)
    qw, pw, f1, f2, qb, pb, f1b, f2b, n1g, n1o, n2g, n2o, tab_out = call(
        final_kernel,
        [shape((36, C), F32), shape((12, C), F32), shape((48, C), F32), shape((12, FF), F32),
         shape((36,), F32), shape((12,), F32), shape((48,), F32)] + [shape((12,), F32)] * 5
        + [shape((12 * ROWS, 23), F32)],
        near=2,
    )(parts, tab_all.reshape(16 * SLOT, 128))
    full = both.reshape(2, *grid[1:])
    ends = home.reshape(2, grid[1], grid[2], 8, C)[:, :, :, :6]
    full = jnp.concatenate([ends, full[:, :, :, 6:]], axis=3)
    return (full[0][None], full[1][None], qw.T, qb, pw.T, pb, f1.T, f1b, f2.T, f2b, n1g, n1o, n2g, n2o,
            tab_out.reshape(bias_table.shape))


def solution(mesh):
    split = Mesh(mesh.devices.reshape(16, 4, 2, 2), ("lon", "y", "core", "ens"))
    lat = ("y", "core")
    tokens = P("ens", None, lat, "lon", None)
    table = P(None, lat, None, None, None, None)
    return jax.shard_map(
        on_device,
        mesh=split,
        in_specs=(tokens, tokens, P(), P(), P(), P(), table) + (P(),) * 8,
        out_specs=(tokens, tokens, P(None, "lon"), P("lon"), P(None, "lon"), P("lon"), P(None, "lon"),
                   P("lon"), P(None, "lon"), P("lon"), P("lon"), P("lon"), P("lon"), P("lon"), table),
        check_vma=False,
    )
```

```python
import math

import jax
import jax.numpy as jnp
from jax import lax
from jax.experimental import pallas as pl
from jax.experimental.pallas import tpu as pltpu
from jax.sharding import Mesh
from jax.sharding import PartitionSpec as P

C = 192
HEADS = 6
FF = 768
ROWS = 144
LANES = 896
HX = 72
TAB = 384
EPS = 1e-05
SCALE = 32 ** -0.5
F32 = jnp.float32
BF16 = jnp.bfloat16
FACTOR = 1.0 / math.sqrt(147456)
GELU_A = 0.044715
GELU_C = math.sqrt(2.0 / math.pi)
PART = 112
SLOT = 32


def nn(a, b):
    return lax.dot_general(a, b, (((1,), (0,)), ((), ())), preferred_element_type=F32)


def nt(a, b):
    return lax.dot_general(a, b, (((1,), (1,)), ((), ())), preferred_element_type=F32)


def tn(a, b):
    return lax.dot_general(a, b, (((0,), (0,)), ((), ())), preferred_element_type=F32)


def iota(dims, axis):
    return lax.broadcasted_iota(jnp.int32, dims, axis).astype(F32)


def whole(value, size):
    return jnp.floor((value + 0.5) * (1.0 / size))


def one_hot(hit):
    return jnp.where(hit, 1.0, 0.0).astype(BF16)


def prep_kernel(qkv_hbm, proj_hbm, fc1_hbm, fc2_hbm, tab_hbm,
                wt_ref, projb_ref, fc1b_ref, fc2b_ref, bias_ref, spread_ref, mask_ref, sel_ref,
                ra_ref, ca_ref, rb_ref, cb_ref,
                qkv_ref, proj_ref, fc1_ref, fc2_ref, tab_ref, sems):
    copies = [
        pltpu.make_async_copy(src, dst, sems.at[k])
        for k, (src, dst) in enumerate(
            ((tab_hbm, tab_ref), (qkv_hbm, qkv_ref), (proj_hbm, proj_ref), (fc1_hbm, fc1_ref),
             (fc2_hbm, fc2_ref))
        )
    ]
    for copy in copies:
        copy.start()
    lane = iota((8, LANES), 1)
    cell = whole(lane, HX)
    rest = lane - HX * cell
    head = whole(rest, 12)
    token = 12.0 * (rest - 12.0 * head) + cell
    token = jnp.where(lane < 12.0 * HX, token, -1.0)[0:1]
    head = jnp.where(lane < 12.0 * HX, head, -1.0)[0:1]
    spread_ref[...] = one_hot(iota((ROWS, LANES), 0) == token)
    for h in range(HEADS):
        mask_ref[32 * h : 32 * h + 32, :] = one_hot(
            jnp.broadcast_to(head, (32, LANES)) == float(h)
        )
    row = iota((ROWS, 128), 0)
    level = whole(row, 12)
    base = 44.0 * level - row + 11.0
    column_id = iota((ROWS, 128), 1)
    for i in range(12):
        for t in range(3):
            sel_ref[ROWS * i : ROWS * i + ROWS, 128 * t : 128 * t + 128] = one_hot(
                base + float(i) == column_id + 128.0 * t
            )
    n = iota((576, 128), 0)
    spot = iota((576, 128), 1)
    ca_ref[0:576, :] = one_hot(spot == n - 36.0 * whole(n, 36))
    n = iota((768, 128), 0)
    spot = iota((768, 128), 1)
    ca_ref[576:1344, :] = one_hot(spot == n - 48.0 * whole(n, 48) + 36.0)
    n = iota((192, 128), 0)
    spot = iota((192, 128), 1)
    n = n - 12.0 * whole(n, 12)
    for k in range(6):
        cb_ref[192 * k : 192 * k + 192, :] = one_hot(spot == n + 12.0 * k)
    n = iota((16, 1344), 1)
    n = jnp.where(n < 576.0, whole(n, 36), whole(n - 576.0, 48))
    ra_ref[...] = one_hot(n == iota((16, 1344), 0))
    n = iota((16, 1152), 1)
    n = whole(n - 192.0 * whole(n, 192), 12)
    rb_ref[...] = one_hot(n == iota((16, 1152), 0))
    copies[0].wait()
    tiles = []
    for t in range(3):
        tile = None
        for k in range(4):
            piece = tab_ref[pl.ds(4 * t + k, ROWS, stride=12), :]
            piece = jnp.concatenate([piece, jnp.zeros((ROWS, 105), F32)], axis=1)
            if k:
                piece = pltpu.roll(piece, 32 * k, 1)
            tile = piece if tile is None else tile + piece
        tiles.append(tile)
    table = jnp.concatenate(tiles, axis=1)
    high = table.astype(BF16)
    low = (table - high.astype(F32)).astype(BF16)
    pieces = [[], []]
    for i in range(12):
        sel = sel_ref[ROWS * i : ROWS * i + ROWS, :]
        got = nt(sel, high) + nt(sel, low)
        pieces[0].append(got[:, :HX])
        pieces[1].append(got[:, HX:])
    for v in range(2):
        spare = jnp.zeros((ROWS, LANES - 12 * HX), F32)
        bias_ref[v] = jnp.concatenate(pieces[v] + [spare], axis=1)
    copies[1].wait()
    wt_ref[...] = qkv_ref[...].T.astype(BF16)
    copies[2].wait()
    projb_ref[...] = proj_ref[...].astype(BF16)
    copies[3].wait()
    fc1b_ref[...] = fc1_ref[...].astype(BF16)
    copies[4].wait()
    fc2b_ref[...] = fc2_ref[...].astype(BF16)


def column(row):
    size = row.shape[1]
    eye = lax.broadcasted_iota(jnp.int32, (size, size), 0) == lax.broadcasted_iota(
        jnp.int32, (size, size), 1
    )
    return jnp.sum(jnp.where(eye, row, 0.0), axis=1, keepdims=True)


def window_picks():
    r = lax.broadcasted_iota(jnp.int32, (576, 128), 0).astype(F32)
    m = jnp.floor((r + 0.5) * (1.0 / 12.0))
    j = r - 12.0 * m
    second = m >= 24.0
    n = jnp.where(second, m - 24.0, m)
    src = jnp.where(second, 24.0 * n + 18.0 + j, 24.0 * n + 6.0 + j)
    src = jnp.where(second & (j >= 6.0), 570.0 + 8.0 * n + j, src)
    lane = lax.broadcasted_iota(jnp.int32, (576, 128), 1).astype(F32)
    tiles = [jnp.where(src == lane + 128.0 * t, 1.0, 0.0).astype(BF16) for t in range(6)]
    return jnp.concatenate(tiles, axis=1)


def natural_picks():
    p = lax.broadcasted_iota(jnp.int32, (768, 128), 0).astype(F32)
    own = p < 576.0
    q = p - 576.0
    n = jnp.where(own, jnp.floor((p + 0.5) * (1.0 / 24.0)), jnp.floor((q + 0.5) * 0.125))
    c = jnp.where(own, p - 24.0 * n, q - 8.0 * n)
    inner = jnp.where(c < 18.0, 12.0 * n + c - 6.0, 288.0 + 12.0 * n + c - 18.0)
    inner = jnp.where(c < 6.0, -1.0, inner)
    outer = jnp.where(c < 6.0, 294.0 + 12.0 * n + c, -1.0)
    dst = jnp.where(own, inner, outer)
    lane = lax.broadcasted_iota(jnp.int32, (768, 128), 1).astype(F32)
    tiles = [jnp.where(dst == lane + 128.0 * t, 1.0, 0.0).astype(BF16) for t in range(5)]
    return jnp.concatenate(tiles, axis=1)[:, :576]


def norm_parts(values):
    centre = jnp.sum(values, axis=1, keepdims=True) * (1.0 / C)
    centred = values - centre
    spread = jnp.sum(centred * centred, axis=1, keepdims=True) * (1.0 / C)
    inverse = lax.rsqrt(spread + EPS)
    return centred * inverse, inverse


def norm_back(grad, hat, inverse, gain):
    scaled = grad * gain
    first = jnp.sum(scaled, axis=1, keepdims=True) * (1.0 / C)
    second = jnp.sum(scaled * hat, axis=1, keepdims=True) * (1.0 / C)
    return inverse * (scaled - first - hat * second)


def front_kernel(x_ref, cot_ref, n1g_ref, n1o_ref, qb_ref, pb_ref, n2g_ref, n2o_ref,
                 f1b_ref, f2b_ref, halo_ref, bias_ref, wt_ref, proj_ref, fc1_ref, fc2_ref,
                 spread_ref, mask_ref, sel_ref,
                 low_ref, block_ref, few_ref, wide_ref, hat_ref, inv_ref, rg_ref, row_ref, f1s_ref,
                 sum_ref, tab_ref):
    n1g, n1o, qb, pb, n2g, n2o, f1b, f2b = (
        ref[...].reshape(1, -1)
        for ref in (n1g_ref, n1o_ref, qb_ref, pb_ref, n2g_ref, n2o_ref, f1b_ref, f2b_ref)
    )
    picks = window_picks()
    xw = nn(picks, jnp.concatenate([x_ref[...], halo_ref[0]], axis=0))
    cw = nn(picks, jnp.concatenate([cot_ref[...], halo_ref[1]], axis=0))
    cot_low = cw.astype(BF16)
    hat1, inv1 = norm_parts(xw)
    normed = (hat1 * n1g + n1o).astype(BF16)
    wq = wt_ref[0:192, :]
    wk = wt_ref[192:384, :]
    wv = wt_ref[384:576, :]
    bq_row = qb[:, 0:192]
    bk_row = qb[:, 192:384]
    bv_row = qb[:, 384:576]
    bq = column(bq_row)
    bk = column(bk_row)
    bv = column(bv_row)
    keys = (nt(normed, wk) + bk_row).astype(BF16)
    values = (nt(normed, wv) + bv_row).astype(BF16)
    spread = spread_ref[...]
    mask = mask_ref[...]
    saved = []
    attended = []
    for g in range(4):
        rows = slice(ROWS * g, ROWS * g + ROWS)
        own = normed[rows]
        query_t = (nt(wq, own) + bq).astype(BF16)
        value_t = (nt(wv, own) + bv).astype(BF16)
        query_bd = nn(query_t, spread).astype(BF16) * mask
        scores = nn(keys[rows], query_bd) * SCALE + bias_ref[g % 2]
        peak = jnp.max(scores, axis=0, keepdims=True)
        raised = jnp.exp(scores - peak)
        total = jnp.sum(raised, axis=0, keepdims=True)
        weights = (raised * (1.0 / total)).astype(BF16)
        mixed = nn(value_t, weights).astype(BF16) * mask
        attended.append(nt(spread, mixed).astype(BF16))
        saved.append((query_bd, weights))
    attended = jnp.concatenate(attended, axis=0)
    attn_out = (nn(attended, proj_ref[...]) + pb).astype(BF16)
    resid = xw + attn_out.astype(F32)
    hat2, inv2 = norm_parts(resid)
    normed2 = (hat2 * n2g + n2o).astype(BF16)
    acts = []
    grads = []
    f1_sums = []
    for g in range(4):
        rows = slice(ROWS * g, ROWS * g + ROWS)
        u = nn(normed2[rows], fc1_ref[...]) + f1b
        square = u * u
        t = jnp.tanh(GELU_C * (u + GELU_A * (square * u)))
        half = 0.5 * (1.0 + t)
        acts.append((u * half).astype(BF16))
        slope = half + 0.5 * u * (1.0 - t * t) * (GELU_C + (3.0 * GELU_A * GELU_C) * square)
        act_grad = nn(cot_low[rows], fc2_ref[...])
        pre = (act_grad * slope).astype(BF16)
        grads.append(pre)
        f1_sums.append(jnp.sum(pre.astype(F32), axis=0, keepdims=True))
    activated = jnp.concatenate(acts, axis=0)
    pre_grad = jnp.concatenate(grads, axis=0)
    f1_sum = f1_sums[0] + f1_sums[1] + f1_sums[2] + f1_sums[3]
    block = (resid + nt(activated, fc2_ref[...]) + f2b).astype(BF16)
    block_ref[...] = block
    n2_grad = nt(pre_grad, fc1_ref[...])
    n2g_sum = jnp.sum(n2_grad * hat2, axis=0, keepdims=True)
    n2o_sum = jnp.sum(n2_grad, axis=0, keepdims=True)
    resid_grad = cw + norm_back(n2_grad, hat2, inv2, n2g)
    attn_grad = resid_grad.astype(BF16)
    pb_sum = jnp.sum(attn_grad.astype(F32), axis=0, keepdims=True)
    f2_sum = jnp.sum(cw, axis=0, keepdims=True)
    grad_q = []
    grad_k = []
    grad_v = []
    for g in range(4):
        rows = slice(ROWS * g, ROWS * g + ROWS)
        query_bd, weights = saved[g]
        own = normed[rows]
        grad_t = nt(proj_ref[...], attn_grad[rows]).astype(BF16)
        grad_bd = nn(grad_t, spread).astype(BF16) * mask
        prob_grad = nn(values[rows], grad_bd)
        probs = weights.astype(F32)
        shared = jnp.sum(probs * prob_grad, axis=0, keepdims=True)
        score_grad = probs * (prob_grad - shared)
        if g < 2:
            sum_ref[g] = score_grad
        else:
            sum_ref[g - 2] += score_grad
        low = score_grad.astype(BF16)
        grad_v.append(nt(weights, grad_bd).astype(BF16))
        grad_k.append((nt(low, query_bd) * SCALE).astype(BF16))
        key_t = (nt(wk, own) + bk).astype(BF16)
        mixed = (nn(key_t, low) * SCALE).astype(BF16) * mask
        grad_q.append(nt(spread, mixed).astype(BF16))
    for v in range(2):
        turned = sum_ref[v].T
        total = jnp.zeros((HX, TAB), F32)
        for i in range(12):
            piece = turned[HX * i : HX * i + HX, :].astype(BF16)
            total = total + nn(piece, sel_ref[ROWS * i : ROWS * i + ROWS, :])
        for t in range(3):
            tab_ref[ROWS * t + HX * v : ROWS * t + HX * v + HX, :] = total[:, 128 * t : 128 * t + 128]
    tab_ref[3 * ROWS :, :] = jnp.zeros((16 * SLOT - 3 * ROWS, 128), F32)
    low_ref[...] = tab_ref[...].astype(BF16)
    for k, group in enumerate((grad_q, grad_k, grad_v)):
        for g in range(4):
            few_ref[k, ROWS * g : ROWS * g + ROWS, :] = group[g]
    few_ref[3] = normed
    few_ref[4] = normed2
    few_ref[5] = cot_low
    few_ref[6] = attn_grad
    few_ref[7] = attended
    wide_ref[0] = pre_grad
    wide_ref[1] = activated
    hat_ref[...] = hat1
    inv_ref[...] = inv1
    rg_ref[...] = resid_grad
    row_ref[0:1, :] = pb_sum
    row_ref[1:2, :] = f2_sum
    row_ref[2:3, :] = n2g_sum
    row_ref[3:4, :] = n2o_sum
    f1s_ref[...] = f1_sum


def back_kernel(core_ref, n1g_ref, block_ref, few_ref, wide_ref, hat_ref, inv_ref, rg_ref, row_ref,
                f1s_ref, wt_ref, ra_ref, ca_ref, rb_ref, cb_ref,
                out_ref, edge_ref, own_ref, send_ref, stage_ref):
    wq = wt_ref[0:192, :]
    wk = wt_ref[192:384, :]
    wv = wt_ref[384:576, :]
    n1g = n1g_ref[...].reshape(1, -1)
    dq = few_ref[0]
    dk = few_ref[1]
    dv = few_ref[2]
    normed = few_ref[3]
    hat1 = hat_ref[...]
    f1_sum = f1s_ref[...]
    pb_sum = row_ref[0:1, :]
    f2_sum = row_ref[1:2, :]
    n2g_sum = row_ref[2:3, :]
    n2o_sum = row_ref[3:4, :]
    back = natural_picks()
    placed = nn(back, block_ref[...]).astype(BF16)
    out_ref[0] = placed[:576]
    edge_ref[0] = placed[576:]
    n1_grad = nn(dq, wq) + nn(dk, wk) + nn(dv, wv)
    n1g_sum = jnp.sum(n1_grad * hat1, axis=0, keepdims=True)
    n1o_sum = jnp.sum(n1_grad, axis=0, keepdims=True)
    input_grad = (rg_ref[...] + norm_back(n1_grad, hat1, inv_ref[...], n1g)).astype(BF16)
    placed = nn(back, input_grad).astype(BF16)
    out_ref[1] = placed[:576]
    edge_ref[1] = placed[576:]
    sums = [jnp.sum(d.astype(F32), axis=0, keepdims=True) for d in (dq, dk, dv)]
    dw_q = tn(dq, normed)
    dw_k = tn(dk, normed)
    dw_v = tn(dv, normed)
    dw_qkv = jnp.concatenate([dw_q, dw_k, dw_v], axis=0)
    dw_p = tn(few_ref[6], few_ref[7])
    dw_1 = tn(wide_ref[0], few_ref[4])
    dw_2 = tn(few_ref[5], wide_ref[1])
    vec_a = jnp.concatenate(sums + [f1_sum[:, 0:192], f1_sum[:, 192:384], f1_sum[:, 384:576], f1_sum[:, 576:768]], axis=1)
    vec_b = jnp.concatenate([pb_sum, f2_sum, n1g_sum, n1o_sum, n2g_sum, n2o_sum], axis=1)
    row_a = nn((ra_ref[...].astype(F32) * vec_a).astype(BF16), ca_ref[...])
    row_b = nn((rb_ref[...].astype(F32) * vec_b).astype(BF16), cb_ref[...])
    for l in range(16):
        a36 = dw_qkv[36 * l : 36 * l + 36]
        a12 = dw_p[12 * l : 12 * l + 12]
        b48 = dw_1[48 * l : 48 * l + 48]
        d12 = dw_2[12 * l : 12 * l + 12]
        top = PART * l
        stage_ref[0, top : top + 36, :] = a36[:, :128]
        stage_ref[0, top + 36 : top + 48, :] = a12[:, :128]
        a_rest = jnp.concatenate([a36[:, 128:], a12[:, 128:]], axis=0)
        stage_ref[0, top + 48 : top + 96, :] = jnp.concatenate([a_rest, b48[:, 128:]], axis=1)
        stage_ref[0, top + 96 : top + 108, :] = d12[:, 640:]
        stage_ref[0, top + 108 : top + 109, :] = row_a[l : l + 1]
        stage_ref[0, top + 109 : top + 110, :] = row_b[l : l + 1]
        stage_ref[0, top + 110 : top + 112, :] = jnp.zeros((2, 128), F32)
        stage_ref[1, top : top + 48, :] = b48[:, :128]
        for b in range(5):
            stage_ref[1, top + 48 + 12 * b : top + 60 + 12 * b, :] = d12[:, 128 * b : 128 * b + 128]
        stage_ref[1, top + 108 : top + 112, :] = jnp.zeros((4, 128), F32)
    core = core_ref[0]
    own_ref[...] = stage_ref[core].astype(BF16)
    send_ref[...] = stage_ref[1 - core].astype(BF16)


def join_kernel(own_ref, got_ref, tab_ref, twin_ref, out_ref):
    for l in range(16):
        part = slice(PART * l, PART * l + PART)
        out_ref[l, 0:PART, :] = (own_ref[part].astype(F32) + got_ref[part].astype(F32)).astype(BF16)
        spot = slice(SLOT * l, SLOT * l + SLOT)
        out_ref[l, PART:, :] = (tab_ref[spot].astype(F32) + twin_ref[spot].astype(F32)).astype(BF16)


def lon_sum_kernel(in_ref, part_ref, tab_ref):
    total = in_ref[0].astype(F32)
    for l in range(1, 16):
        total = total + in_ref[l].astype(F32)
    low = total.astype(BF16)
    part_ref[...] = low[:PART]
    for k in range(16):
        tab_ref[k] = low[PART:]


def band_sum_kernel(slot_ref, *refs):
    out_ref, all_ref = refs[8], refs[9]
    slot = slot_ref[0]
    for k in range(8):
        all_ref[jnp.bitwise_xor(slot, k)] = refs[k][...].astype(F32)
    total = all_ref[0]
    for k in range(1, 8):
        total = total + all_ref[k]
    out_ref[...] = total.astype(BF16)


def weight_kernel(core_ref, own_ref, got_ref, qw_ref, pw_ref, f1_ref, f2_ref, qb_ref, pb_ref, f1b_ref,
                  f2b_ref, n1g_ref, n1o_ref, n2g_ref, n2o_ref, pair_ref):
    core = core_ref[0]
    pair_ref[core] = own_ref[...].astype(F32) * FACTOR
    pair_ref[1 - core] = got_ref[...].astype(F32) * FACTOR
    first = pair_ref[0]
    second = pair_ref[1]
    a = jnp.concatenate([first[0:48], first[48:96, 0:64]], axis=1)
    qw_ref[...] = a[0:36]
    pw_ref[...] = a[36:48]
    f1_ref[...] = jnp.concatenate([second[0:48], first[48:96, 64:128]], axis=1)
    d = [second[48 + 12 * k : 60 + 12 * k] for k in range(5)] + [first[96:108]]
    f2_ref[...] = jnp.concatenate(d, axis=1)
    va = first[108:109]
    vb = first[109:110]
    qb_ref[...] = va[:, 0:36].reshape(36)
    f1b_ref[...] = va[:, 36:84].reshape(48)
    for k, ref in enumerate((pb_ref, f2b_ref, n1g_ref, n1o_ref, n2g_ref, n2o_ref)):
        ref[...] = vb[:, 12 * k : 12 * k + 12].reshape(12)


def table_kernel(tab_ref, out_tab_ref):
    tab = tab_ref[...].astype(F32)
    for t in range(3):
        tile = tab[ROWS * t : ROWS * t + ROWS]
        for k in range(4):
            piece = pltpu.roll(tile, 128 - 32 * k, 1) if k else tile
            out_tab_ref[pl.ds(4 * t + k, ROWS, stride=12), :] = piece[:, :23]


def call(kernel, out_shape, smem=0, far=0, near=0, limit=8, scratch=(), raw=False, flops=0):
    count = smem + far + near
    space = pltpu.HBM if raw else pltpu.VMEM
    specs = [pl.BlockSpec(memory_space=pltpu.SMEM)] * smem + [
        pl.BlockSpec(memory_space=space)
    ] * (far + near)
    run = pl.pallas_call(
        kernel,
        out_shape=out_shape,
        in_specs=specs,
        out_specs=jax.tree.map(lambda _: pl.BlockSpec(memory_space=pltpu.VMEM), out_shape),
        scratch_shapes=scratch,
        compiler_params=pltpu.CompilerParams(vmem_limit_bytes=limit << 20),
        cost_estimate=pl.CostEstimate(flops=flops, transcendentals=0, bytes_accessed=0)
        if flops
        else None,
    )

    def go(*args):
        if raw:
            args = tuple(pltpu.with_memory_space_constraint(a, pltpu.HBM) for a in args)
        kept = args[: smem + far] + tuple(
            pltpu.with_memory_space_constraint(a, pltpu.VMEM) for a in args[smem + far :]
        )
        assert len(args) == count
        return run(*kept)

    return go


def near(dims, dtype):
    return pltpu.VMEM(dims, dtype)


def shape(dims, dtype):
    return jax.ShapeDtypeStruct(dims, dtype)


def on_device(inputs, cotangent, norm1_gain, norm1_offset, qkv_weight, qkv_bias, bias_table,
              proj_weight, proj_bias, norm2_gain, norm2_offset, fc1_weight, fc1_bias,
              fc2_weight, fc2_bias):
    grid = inputs.shape
    x = inputs.reshape(576, C)
    cot = cotangent.reshape(576, C)
    edge = jnp.stack([inputs[0, :, :, :8, :].reshape(192, C), cotangent[0, :, :, :8, :].reshape(192, C)])
    halo = lax.ppermute(edge, "lon", [(k, (k - 1) % 16) for k in range(16)])
    table = bias_table.reshape(12 * ROWS, 23)
    wt, proj, fc1, fc2, bias, spread, mask, sel, ra, ca, rb, cb = call(
        prep_kernel,
        [near((576, C), BF16), near((C, C), BF16), near((C, FF), BF16), near((C, FF), BF16),
         near((2, ROWS, LANES), F32), near((ROWS, LANES), BF16), near((C, LANES), BF16),
         near((12 * ROWS, TAB), BF16), near((16, 1344), BF16), near((1344, 128), BF16),
         near((16, 1152), BF16), near((1152, 128), BF16)],
        far=5,
        limit=16,
        raw=True,
        scratch=[pltpu.VMEM((C, 576), F32), pltpu.VMEM((C, C), F32), pltpu.VMEM((C, FF), F32),
                 pltpu.VMEM((C, FF), F32), pltpu.VMEM((12 * ROWS, 23), F32),
                 pltpu.SemaphoreType.DMA((5,))],
    )(qkv_weight, proj_weight, fc1_weight, fc2_weight.T, table)
    core = lax.axis_index("core").astype(jnp.int32).reshape(1)
    slot = (2 * lax.axis_index("y") + lax.axis_index("ens")).astype(jnp.int32).reshape(1)
    tab, *state = call(
        front_kernel,
        [near((16 * SLOT, 128), BF16), near((576, C), BF16), near((8, 576, C), BF16),
         near((2, 576, FF), BF16), near((576, C), F32), near((576, 1), F32), near((576, C), F32),
         near((8, C), F32), near((1, FF), F32)],
        far=10,
        near=9,
        limit=24,
        scratch=[pltpu.VMEM((2, ROWS, LANES), F32), pltpu.VMEM((16 * SLOT, 128), F32)],
    )(x, cot, norm1_gain, norm1_offset, qkv_bias, proj_bias, norm2_gain, norm2_offset, fc1_bias,
      fc2_bias, halo, bias, wt, proj, fc1, fc2, spread, mask, sel)
    twin = lax.ppermute(tab, "ens", [(0, 1), (1, 0)])
    both, ends, own, send = call(
        back_kernel,
        [shape((2, 576, C), BF16), near((2, 192, C), BF16), near((16 * PART, 128), BF16),
         near((16 * PART, 128), BF16)],
        smem=1,
        far=1,
        near=13,
        limit=16,
        scratch=[pltpu.VMEM((2, 16 * PART, 128), F32)],
    )(core, norm1_gain, *state, wt, ra, ca, rb, cb)
    got = lax.ppermute(send, "core", [(0, 1), (1, 0)])
    home = lax.ppermute(ends, "lon", [(k, (k + 1) % 16) for k in range(16)])
    joined = call(join_kernel, near((16, PART + SLOT, 128), BF16), near=4)(own, got, tab, twin)
    arrived = lax.all_to_all(joined, "lon", split_axis=0, concat_axis=0, tiled=True)
    part, tab_copies = call(
        lon_sum_kernel, [near((PART, 128), BF16), near((16, SLOT, 128), BF16)], near=1
    )(arrived)
    bands = [part] + [
        lax.ppermute(part, ("y", "ens"), [(n, n ^ k) for n in range(8)]) for k in range(1, 8)
    ]
    tab_all = lax.all_to_all(tab_copies, "lon", split_axis=0, concat_axis=0, tiled=True)
    half = call(
        band_sum_kernel, near((PART, 128), BF16), smem=1, near=8,
        scratch=[pltpu.VMEM((8, PART, 128), F32)],
    )(slot, *bands)
    other = lax.ppermute(half, "core", [(0, 1), (1, 0)])
    qw, pw, f1, f2, qb, pb, f1b, f2b, n1g, n1o, n2g, n2o = call(
        weight_kernel,
        [shape((36, C), F32), shape((12, C), F32), shape((48, C), F32), shape((12, FF), F32),
         shape((36,), F32), shape((12,), F32), shape((48,), F32)] + [shape((12,), F32)] * 5,
        smem=1,
        near=2,
        scratch=[pltpu.VMEM((2, PART, 128), F32)],
    )(core, half, other)
    tab_out = call(table_kernel, shape((12 * ROWS, 23), F32), near=1)(
        tab_all.reshape(16 * SLOT, 128)
    )
    full = both.reshape(2, *grid[1:])
    ends = home.reshape(2, grid[1], grid[2], 8, C)[:, :, :, :6]
    full = jnp.concatenate([ends, full[:, :, :, 6:]], axis=3)
    return (full[0][None], full[1][None], qw.T, qb, pw.T, pb, f1.T, f1b, f2.T, f2b, n1g, n1o, n2g, n2o,
            tab_out.reshape(bias_table.shape))


def solution(mesh):
    split = Mesh(mesh.devices.reshape(16, 4, 2, 2), ("lon", "y", "core", "ens"))
    lat = ("y", "core")
    tokens = P("ens", None, lat, "lon", None)
    table = P(None, lat, None, None, None, None)
    return jax.shard_map(
        on_device,
        mesh=split,
        in_specs=(tokens, tokens, P(), P(), P(), P(), table) + (P(),) * 8,
        out_specs=(tokens, tokens, P(None, "lon"), P("lon"), P(None, "lon"), P("lon"), P(None, "lon"),
                   P("lon"), P(None, "lon"), P("lon"), P("lon"), P("lon"), P("lon"), P("lon"), table),
        check_vma=False,
    )
```

```python
import math

import jax
import jax.numpy as jnp
from jax import lax
from jax.experimental import pallas as pl
from jax.experimental.pallas import tpu as pltpu
from jax.sharding import Mesh
from jax.sharding import PartitionSpec as P

C = 192
HEADS = 6
FF = 768
ROWS = 144
LANES = 896
HX = 72
TAB = 384
EPS = 1e-05
SCALE = 32 ** -0.5
F32 = jnp.float32
BF16 = jnp.bfloat16
FACTOR = 1.0 / math.sqrt(147456)
GELU_A = 0.044715
GELU_C = math.sqrt(2.0 / math.pi)
PART = 112
SLOT = 32


def nn(a, b):
    return lax.dot_general(a, b, (((1,), (0,)), ((), ())), preferred_element_type=F32)


def nt(a, b):
    return lax.dot_general(a, b, (((1,), (1,)), ((), ())), preferred_element_type=F32)


def tn(a, b):
    return lax.dot_general(a, b, (((0,), (0,)), ((), ())), preferred_element_type=F32)


def iota(dims, axis):
    return lax.broadcasted_iota(jnp.int32, dims, axis).astype(F32)


def whole(value, size):
    return jnp.floor((value + 0.5) * (1.0 / size))


def one_hot(hit):
    return jnp.where(hit, 1.0, 0.0).astype(BF16)


def prep_kernel(qkv_hbm, proj_hbm, fc1_hbm, fc2_hbm, tab_hbm,
                wt_ref, projb_ref, fc1b_ref, fc2b_ref, bias_ref, spread_ref, mask_ref, sel_ref,
                ra_ref, ca_ref, rb_ref, cb_ref, picks_ref, back_ref,
                qkv_ref, proj_ref, fc1_ref, fc2_ref, tab_ref, sems):
    copies = [
        pltpu.make_async_copy(src, dst, sems.at[k])
        for k, (src, dst) in enumerate(
            ((tab_hbm, tab_ref), (qkv_hbm, qkv_ref), (proj_hbm, proj_ref), (fc1_hbm, fc1_ref),
             (fc2_hbm, fc2_ref))
        )
    ]
    for copy in copies:
        copy.start()
    lane = iota((8, LANES), 1)
    cell = whole(lane, HX)
    rest = lane - HX * cell
    head = whole(rest, 12)
    token = 12.0 * (rest - 12.0 * head) + cell
    token = jnp.where(lane < 12.0 * HX, token, -1.0)[0:1]
    head = jnp.where(lane < 12.0 * HX, head, -1.0)[0:1]
    spread_ref[...] = one_hot(iota((ROWS, LANES), 0) == token)
    for h in range(HEADS):
        mask_ref[32 * h : 32 * h + 32, :] = one_hot(
            jnp.broadcast_to(head, (32, LANES)) == float(h)
        )
    row = iota((ROWS, 128), 0)
    level = whole(row, 12)
    base = 44.0 * level - row + 11.0
    column_id = iota((ROWS, 128), 1)
    for i in range(12):
        for t in range(3):
            sel_ref[ROWS * i : ROWS * i + ROWS, 128 * t : 128 * t + 128] = one_hot(
                base + float(i) == column_id + 128.0 * t
            )
    n = iota((576, 128), 0)
    spot = iota((576, 128), 1)
    ca_ref[0:576, :] = one_hot(spot == n - 36.0 * whole(n, 36))
    n = iota((768, 128), 0)
    spot = iota((768, 128), 1)
    ca_ref[576:1344, :] = one_hot(spot == n - 48.0 * whole(n, 48) + 36.0)
    n = iota((192, 128), 0)
    spot = iota((192, 128), 1)
    n = n - 12.0 * whole(n, 12)
    for k in range(6):
        cb_ref[192 * k : 192 * k + 192, :] = one_hot(spot == n + 12.0 * k)
    n = iota((16, 1344), 1)
    n = jnp.where(n < 576.0, whole(n, 36), whole(n - 576.0, 48))
    ra_ref[...] = one_hot(n == iota((16, 1344), 0))
    n = iota((16, 1152), 1)
    n = whole(n - 192.0 * whole(n, 192), 12)
    rb_ref[...] = one_hot(n == iota((16, 1152), 0))
    picks_ref[...] = window_picks()
    back_ref[...] = natural_picks()
    copies[0].wait()
    tiles = []
    for t in range(3):
        tile = None
        for k in range(4):
            piece = tab_ref[pl.ds(4 * t + k, ROWS, stride=12), :]
            piece = jnp.concatenate([piece, jnp.zeros((ROWS, 105), F32)], axis=1)
            if k:
                piece = pltpu.roll(piece, 32 * k, 1)
            tile = piece if tile is None else tile + piece
        tiles.append(tile)
    table = jnp.concatenate(tiles, axis=1)
    high = table.astype(BF16)
    low = (table - high.astype(F32)).astype(BF16)
    pieces = [[], []]
    for i in range(12):
        sel = sel_ref[ROWS * i : ROWS * i + ROWS, :]
        got = nt(sel, high) + nt(sel, low)
        pieces[0].append(got[:, :HX])
        pieces[1].append(got[:, HX:])
    for v in range(2):
        spare = jnp.zeros((ROWS, LANES - 12 * HX), F32)
        bias_ref[v] = jnp.concatenate(pieces[v] + [spare], axis=1)
    copies[1].wait()
    wt_ref[...] = qkv_ref[...].T.astype(BF16)
    copies[2].wait()
    projb_ref[...] = proj_ref[...].astype(BF16)
    copies[3].wait()
    fc1b_ref[...] = fc1_ref[...].astype(BF16)
    copies[4].wait()
    fc2b_ref[...] = fc2_ref[...].astype(BF16)


def column(row):
    size = row.shape[1]
    eye = lax.broadcasted_iota(jnp.int32, (size, size), 0) == lax.broadcasted_iota(
        jnp.int32, (size, size), 1
    )
    return jnp.sum(jnp.where(eye, row, 0.0), axis=1, keepdims=True)


def window_picks():
    r = lax.broadcasted_iota(jnp.int32, (576, 128), 0).astype(F32)
    m = jnp.floor((r + 0.5) * (1.0 / 12.0))
    j = r - 12.0 * m
    second = m >= 24.0
    n = jnp.where(second, m - 24.0, m)
    src = jnp.where(second, 24.0 * n + 18.0 + j, 24.0 * n + 6.0 + j)
    src = jnp.where(second & (j >= 6.0), 570.0 + 8.0 * n + j, src)
    lane = lax.broadcasted_iota(jnp.int32, (576, 128), 1).astype(F32)
    tiles = [jnp.where(src == lane + 128.0 * t, 1.0, 0.0).astype(BF16) for t in range(6)]
    return jnp.concatenate(tiles, axis=1)


def natural_picks():
    p = lax.broadcasted_iota(jnp.int32, (768, 128), 0).astype(F32)
    own = p < 576.0
    q = p - 576.0
    n = jnp.where(own, jnp.floor((p + 0.5) * (1.0 / 24.0)), jnp.floor((q + 0.5) * 0.125))
    c = jnp.where(own, p - 24.0 * n, q - 8.0 * n)
    inner = jnp.where(c < 18.0, 12.0 * n + c - 6.0, 288.0 + 12.0 * n + c - 18.0)
    inner = jnp.where(c < 6.0, -1.0, inner)
    outer = jnp.where(c < 6.0, 294.0 + 12.0 * n + c, -1.0)
    dst = jnp.where(own, inner, outer)
    lane = lax.broadcasted_iota(jnp.int32, (768, 128), 1).astype(F32)
    tiles = [jnp.where(dst == lane + 128.0 * t, 1.0, 0.0).astype(BF16) for t in range(5)]
    return jnp.concatenate(tiles, axis=1)[:, :576]


def norm_parts(values):
    centre = jnp.sum(values, axis=1, keepdims=True) * (1.0 / C)
    centred = values - centre
    spread = jnp.sum(centred * centred, axis=1, keepdims=True) * (1.0 / C)
    inverse = lax.rsqrt(spread + EPS)
    return centred * inverse, inverse


def norm_back(grad, hat, inverse, gain):
    scaled = grad * gain
    first = jnp.sum(scaled, axis=1, keepdims=True) * (1.0 / C)
    second = jnp.sum(scaled * hat, axis=1, keepdims=True) * (1.0 / C)
    return inverse * (scaled - first - hat * second)


def front_kernel(x_ref, cot_ref, n1g_ref, n1o_ref, qb_ref, pb_ref, n2g_ref, n2o_ref,
                 f1b_ref, f2b_ref, halo_ref, bias_ref, wt_ref, proj_ref, fc1_ref, fc2_ref,
                 spread_ref, mask_ref, sel_ref, picks_ref,
                 low_ref, block_ref, few_ref, wide_ref, hat_ref, inv_ref, rg_ref, row_ref, f1s_ref,
                 sum_ref, tab_ref):
    n1g, n1o, qb, pb, n2g, n2o, f1b, f2b = (
        ref[...].reshape(1, -1)
        for ref in (n1g_ref, n1o_ref, qb_ref, pb_ref, n2g_ref, n2o_ref, f1b_ref, f2b_ref)
    )
    picks = picks_ref[...]
    xw = nn(picks, jnp.concatenate([x_ref[...], halo_ref[0]], axis=0))
    cw = nn(picks, jnp.concatenate([cot_ref[...], halo_ref[1]], axis=0))
    cot_low = cw.astype(BF16)
    hat1, inv1 = norm_parts(xw)
    normed = (hat1 * n1g + n1o).astype(BF16)
    wq = wt_ref[0:192, :]
    wk = wt_ref[192:384, :]
    wv = wt_ref[384:576, :]
    bq_row = qb[:, 0:192]
    bk_row = qb[:, 192:384]
    bv_row = qb[:, 384:576]
    bq = column(bq_row)
    bk = column(bk_row)
    bv = column(bv_row)
    keys = (nt(normed, wk) + bk_row).astype(BF16)
    values = (nt(normed, wv) + bv_row).astype(BF16)
    spread = spread_ref[...]
    mask = mask_ref[...]
    saved = []
    attended = []
    for g in range(4):
        rows = slice(ROWS * g, ROWS * g + ROWS)
        own = normed[rows]
        query_t = (nt(wq, own) + bq).astype(BF16)
        value_t = (nt(wv, own) + bv).astype(BF16)
        query_bd = nn(query_t, spread).astype(BF16) * mask
        scores = nn(keys[rows], query_bd) * SCALE + bias_ref[g % 2]
        peak = jnp.max(scores, axis=0, keepdims=True)
        raised = jnp.exp(scores - peak)
        total = jnp.sum(raised, axis=0, keepdims=True)
        weights = (raised * (1.0 / total)).astype(BF16)
        mixed = nn(value_t, weights).astype(BF16) * mask
        attended.append(nt(spread, mixed).astype(BF16))
        saved.append((query_bd, weights))
    attended = jnp.concatenate(attended, axis=0)
    attn_out = (nn(attended, proj_ref[...]) + pb).astype(BF16)
    resid = xw + attn_out.astype(F32)
    hat2, inv2 = norm_parts(resid)
    normed2 = (hat2 * n2g + n2o).astype(BF16)
    acts = []
    grads = []
    f1_sums = []
    for g in range(4):
        rows = slice(ROWS * g, ROWS * g + ROWS)
        u = nn(normed2[rows], fc1_ref[...]) + f1b
        square = u * u
        half = 0.5 * jnp.tanh(u * (GELU_C + (GELU_A * GELU_C) * square)) + 0.5
        acts.append((u * half).astype(BF16))
        lean = u * (2.0 * GELU_C + (6.0 * GELU_A * GELU_C) * square)
        slope = half + (half - half * half) * lean
        act_grad = nn(cot_low[rows], fc2_ref[...])
        pre = (act_grad * slope).astype(BF16)
        grads.append(pre)
        f1_sums.append(jnp.sum(pre.astype(F32), axis=0, keepdims=True))
    activated = jnp.concatenate(acts, axis=0)
    pre_grad = jnp.concatenate(grads, axis=0)
    f1_sum = f1_sums[0] + f1_sums[1] + f1_sums[2] + f1_sums[3]
    block = (resid + nt(activated, fc2_ref[...]) + f2b).astype(BF16)
    block_ref[...] = block
    n2_grad = nt(pre_grad, fc1_ref[...])
    n2g_sum = jnp.sum(n2_grad * hat2, axis=0, keepdims=True)
    n2o_sum = jnp.sum(n2_grad, axis=0, keepdims=True)
    resid_grad = cw + norm_back(n2_grad, hat2, inv2, n2g)
    attn_grad = resid_grad.astype(BF16)
    pb_sum = jnp.sum(attn_grad.astype(F32), axis=0, keepdims=True)
    f2_sum = jnp.sum(cw, axis=0, keepdims=True)
    grad_q = []
    grad_k = []
    grad_v = []
    for g in range(4):
        rows = slice(ROWS * g, ROWS * g + ROWS)
        query_bd, weights = saved[g]
        own = normed[rows]
        grad_t = nt(proj_ref[...], attn_grad[rows]).astype(BF16)
        grad_bd = nn(grad_t, spread).astype(BF16) * mask
        prob_grad = nn(values[rows], grad_bd)
        probs = weights.astype(F32)
        shared = jnp.sum(probs * prob_grad, axis=0, keepdims=True)
        score_grad = probs * (prob_grad - shared)
        if g < 2:
            sum_ref[g] = score_grad
        else:
            sum_ref[g - 2] += score_grad
        low = score_grad.astype(BF16)
        grad_v.append(nt(weights, grad_bd).astype(BF16))
        grad_k.append((nt(low, query_bd) * SCALE).astype(BF16))
        key_t = (nt(wk, own) + bk).astype(BF16)
        mixed = (nn(key_t, low) * SCALE).astype(BF16) * mask
        grad_q.append(nt(spread, mixed).astype(BF16))
    for v in range(2):
        turned = sum_ref[v].T
        total = jnp.zeros((HX, TAB), F32)
        for i in range(12):
            piece = turned[HX * i : HX * i + HX, :].astype(BF16)
            total = total + nn(piece, sel_ref[ROWS * i : ROWS * i + ROWS, :])
        for t in range(3):
            tab_ref[ROWS * t + HX * v : ROWS * t + HX * v + HX, :] = total[:, 128 * t : 128 * t + 128]
    tab_ref[3 * ROWS :, :] = jnp.zeros((16 * SLOT - 3 * ROWS, 128), F32)
    low_ref[...] = tab_ref[...].astype(BF16)
    for k, group in enumerate((grad_q, grad_k, grad_v)):
        for g in range(4):
            few_ref[k, ROWS * g : ROWS * g + ROWS, :] = group[g]
    few_ref[3] = normed
    few_ref[4] = normed2
    few_ref[5] = cot_low
    few_ref[6] = attn_grad
    few_ref[7] = attended
    wide_ref[0] = pre_grad
    wide_ref[1] = activated
    hat_ref[...] = hat1
    inv_ref[...] = inv1
    rg_ref[...] = resid_grad
    row_ref[0:1, :] = pb_sum
    row_ref[1:2, :] = f2_sum
    row_ref[2:3, :] = n2g_sum
    row_ref[3:4, :] = n2o_sum
    f1s_ref[...] = f1_sum


def back_kernel(core_ref, n1g_ref, few_ref, wide_ref, hat_ref, inv_ref, rg_ref, row_ref,
                f1s_ref, wt_ref, ra_ref, ca_ref, rb_ref, cb_ref,
                ig_ref, own_ref, send_ref, stage_ref):
    wq = wt_ref[0:192, :]
    wk = wt_ref[192:384, :]
    wv = wt_ref[384:576, :]
    n1g = n1g_ref[...].reshape(1, -1)
    dq = few_ref[0]
    dk = few_ref[1]
    dv = few_ref[2]
    normed = few_ref[3]
    hat1 = hat_ref[...]
    f1_sum = f1s_ref[...]
    pb_sum = row_ref[0:1, :]
    f2_sum = row_ref[1:2, :]
    n2g_sum = row_ref[2:3, :]
    n2o_sum = row_ref[3:4, :]
    n1_grad = nn(dq, wq) + nn(dk, wk) + nn(dv, wv)
    n1g_sum = jnp.sum(n1_grad * hat1, axis=0, keepdims=True)
    n1o_sum = jnp.sum(n1_grad, axis=0, keepdims=True)
    input_grad = (rg_ref[...] + norm_back(n1_grad, hat1, inv_ref[...], n1g)).astype(BF16)
    ig_ref[...] = input_grad
    sums = [jnp.sum(d.astype(F32), axis=0, keepdims=True) for d in (dq, dk, dv)]
    dw_q = tn(dq, normed)
    dw_k = tn(dk, normed)
    dw_v = tn(dv, normed)
    dw_qkv = jnp.concatenate([dw_q, dw_k, dw_v], axis=0)
    dw_p = tn(few_ref[6], few_ref[7])
    dw_1 = tn(wide_ref[0], few_ref[4])
    dw_2 = tn(few_ref[5], wide_ref[1])
    vec_a = jnp.concatenate(sums + [f1_sum[:, 0:192], f1_sum[:, 192:384], f1_sum[:, 384:576], f1_sum[:, 576:768]], axis=1)
    vec_b = jnp.concatenate([pb_sum, f2_sum, n1g_sum, n1o_sum, n2g_sum, n2o_sum], axis=1)
    row_a = nn((ra_ref[...].astype(F32) * vec_a).astype(BF16), ca_ref[...])
    row_b = nn((rb_ref[...].astype(F32) * vec_b).astype(BF16), cb_ref[...])
    for l in range(16):
        a36 = dw_qkv[36 * l : 36 * l + 36]
        a12 = dw_p[12 * l : 12 * l + 12]
        b48 = dw_1[48 * l : 48 * l + 48]
        d12 = dw_2[12 * l : 12 * l + 12]
        top = PART * l
        stage_ref[0, top : top + 36, :] = a36[:, :128]
        stage_ref[0, top + 36 : top + 48, :] = a12[:, :128]
        a_rest = jnp.concatenate([a36[:, 128:], a12[:, 128:]], axis=0)
        stage_ref[0, top + 48 : top + 96, :] = jnp.concatenate([a_rest, b48[:, 128:]], axis=1)
        stage_ref[0, top + 96 : top + 108, :] = d12[:, 640:]
        stage_ref[0, top + 108 : top + 109, :] = row_a[l : l + 1]
        stage_ref[0, top + 109 : top + 110, :] = row_b[l : l + 1]
        stage_ref[0, top + 110 : top + 112, :] = jnp.zeros((2, 128), F32)
        stage_ref[1, top : top + 48, :] = b48[:, :128]
        for b in range(5):
            stage_ref[1, top + 48 + 12 * b : top + 60 + 12 * b, :] = d12[:, 128 * b : 128 * b + 128]
        stage_ref[1, top + 108 : top + 112, :] = jnp.zeros((4, 128), F32)
    core = core_ref[0]
    own_ref[...] = stage_ref[core].astype(BF16)
    send_ref[...] = stage_ref[1 - core].astype(BF16)


def place_kernel(block_ref, ig_ref, back_ref, out_ref, edge_ref):
    back = back_ref[...]
    for k, ref in enumerate((block_ref, ig_ref)):
        placed = nn(back, ref[...]).astype(BF16)
        out_ref[k] = placed[:576]
        edge_ref[k] = placed[576:]


def edge_kernel(x_hbm, cot_hbm, out_ref, sems):
    copies = [
        pltpu.make_async_copy(src.at[:, 0:8, :], out_ref.at[k], sems.at[k])
        for k, src in enumerate((x_hbm, cot_hbm))
    ]
    for copy in copies:
        copy.start()
    for copy in copies:
        copy.wait()


def join_kernel(own_ref, got_ref, tab_ref, twin_ref, out_ref):
    for l in range(16):
        part = slice(PART * l, PART * l + PART)
        out_ref[l, 0:PART, :] = (own_ref[part].astype(F32) + got_ref[part].astype(F32)).astype(BF16)
        spot = slice(SLOT * l, SLOT * l + SLOT)
        out_ref[l, PART:, :] = (tab_ref[spot].astype(F32) + twin_ref[spot].astype(F32)).astype(BF16)


def lon_sum_kernel(in_ref, part_ref, tab_ref):
    total = in_ref[0].astype(F32)
    for l in range(1, 16):
        total = total + in_ref[l].astype(F32)
    low = total.astype(BF16)
    for k in range(8):
        part_ref[k] = low[:PART]
    for k in range(16):
        tab_ref[k] = low[PART:]


def band_sum_kernel(in_ref, out_ref):
    total = in_ref[0].astype(F32)
    for k in range(1, 8):
        total = total + in_ref[k].astype(F32)
    out_ref[...] = total.astype(BF16)


def weight_kernel(core_ref, own_ref, got_ref, qw_ref, pw_ref, f1_ref, f2_ref, qb_ref, pb_ref, f1b_ref,
                  f2b_ref, n1g_ref, n1o_ref, n2g_ref, n2o_ref, pair_ref):
    core = core_ref[0]
    pair_ref[core] = own_ref[...].astype(F32) * FACTOR
    pair_ref[1 - core] = got_ref[...].astype(F32) * FACTOR
    first = pair_ref[0]
    second = pair_ref[1]
    a = jnp.concatenate([first[0:48], first[48:96, 0:64]], axis=1)
    qw_ref[...] = a[0:36]
    pw_ref[...] = a[36:48]
    f1_ref[...] = jnp.concatenate([second[0:48], first[48:96, 64:128]], axis=1)
    d = [second[48 + 12 * k : 60 + 12 * k] for k in range(5)] + [first[96:108]]
    f2_ref[...] = jnp.concatenate(d, axis=1)
    va = first[108:109]
    vb = first[109:110]
    qb_ref[...] = va[:, 0:36].reshape(36)
    f1b_ref[...] = va[:, 36:84].reshape(48)
    for k, ref in enumerate((pb_ref, f2b_ref, n1g_ref, n1o_ref, n2g_ref, n2o_ref)):
        ref[...] = vb[:, 12 * k : 12 * k + 12].reshape(12)


def table_kernel(tab_ref, out_tab_ref):
    tab = tab_ref[...].astype(F32)
    for t in range(3):
        tile = tab[ROWS * t : ROWS * t + ROWS]
        for k in range(4):
            piece = pltpu.roll(tile, 128 - 32 * k, 1) if k else tile
            out_tab_ref[pl.ds(4 * t + k, ROWS, stride=12), :] = piece[:, :23]


def call(kernel, out_shape, smem=0, far=0, near=0, limit=8, scratch=(), raw=False, flops=0):
    count = smem + far + near
    space = pltpu.HBM if raw else pltpu.VMEM
    specs = [pl.BlockSpec(memory_space=pltpu.SMEM)] * smem + [
        pl.BlockSpec(memory_space=space)
    ] * (far + near)
    run = pl.pallas_call(
        kernel,
        out_shape=out_shape,
        in_specs=specs,
        out_specs=jax.tree.map(lambda _: pl.BlockSpec(memory_space=pltpu.VMEM), out_shape),
        scratch_shapes=scratch,
        compiler_params=pltpu.CompilerParams(vmem_limit_bytes=limit << 20),
        cost_estimate=pl.CostEstimate(flops=flops, transcendentals=0, bytes_accessed=0)
        if flops
        else None,
    )

    def go(*args):
        if raw:
            args = tuple(pltpu.with_memory_space_constraint(a, pltpu.HBM) for a in args)
        kept = args[: smem + far] + tuple(
            pltpu.with_memory_space_constraint(a, pltpu.VMEM) for a in args[smem + far :]
        )
        assert len(args) == count
        return run(*kept)

    return go


def near(dims, dtype):
    return pltpu.VMEM(dims, dtype)


def shape(dims, dtype):
    return jax.ShapeDtypeStruct(dims, dtype)


def on_device(inputs, cotangent, norm1_gain, norm1_offset, qkv_weight, qkv_bias, bias_table,
              proj_weight, proj_bias, norm2_gain, norm2_offset, fc1_weight, fc1_bias,
              fc2_weight, fc2_bias):
    grid = inputs.shape
    x = inputs.reshape(576, C)
    cot = cotangent.reshape(576, C)
    edge = call(
        edge_kernel, near((2, 24, 8, C), BF16), far=2, raw=True,
        scratch=[pltpu.SemaphoreType.DMA((2,))],
    )(inputs.reshape(24, 24, C), cotangent.reshape(24, 24, C)).reshape(2, 192, C)
    halo = lax.ppermute(edge, "lon", [(k, (k - 1) % 16) for k in range(16)])
    table = bias_table.reshape(12 * ROWS, 23)
    wt, proj, fc1, fc2, bias, spread, mask, sel, ra, ca, rb, cb, picks, back = call(
        prep_kernel,
        [near((576, C), BF16), near((C, C), BF16), near((C, FF), BF16), near((C, FF), BF16),
         near((2, ROWS, LANES), F32), near((ROWS, LANES), BF16), near((C, LANES), BF16),
         near((12 * ROWS, TAB), BF16), near((16, 1344), BF16), near((1344, 128), BF16),
         near((16, 1152), BF16), near((1152, 128), BF16), near((576, 768), BF16), near((768, 576), BF16)],
        far=5,
        limit=16,
        raw=True,
        scratch=[pltpu.VMEM((C, 576), F32), pltpu.VMEM((C, C), F32), pltpu.VMEM((C, FF), F32),
                 pltpu.VMEM((C, FF), F32), pltpu.VMEM((12 * ROWS, 23), F32),
                 pltpu.SemaphoreType.DMA((5,))],
    )(qkv_weight, proj_weight, fc1_weight, fc2_weight.T, table)
    core = lax.axis_index("core").astype(jnp.int32).reshape(1)
    tab, block, *state = call(
        front_kernel,
        [near((16 * SLOT, 128), BF16), near((576, C), BF16), near((8, 576, C), BF16),
         near((2, 576, FF), BF16), near((576, C), F32), near((576, 1), F32), near((576, C), F32),
         near((8, C), F32), near((1, FF), F32)],
        far=10,
        near=10,
        limit=24,
        scratch=[pltpu.VMEM((2, ROWS, LANES), F32), pltpu.VMEM((16 * SLOT, 128), F32)],
    )(x, cot, norm1_gain, norm1_offset, qkv_bias, proj_bias, norm2_gain, norm2_offset, fc1_bias,
      fc2_bias, halo, bias, wt, proj, fc1, fc2, spread, mask, sel, picks)
    twin = lax.ppermute(tab, "ens", [(0, 1), (1, 0)])
    slope, own, send = call(
        back_kernel,
        [near((576, C), BF16), near((16 * PART, 128), BF16), near((16 * PART, 128), BF16)],
        smem=1,
        far=1,
        near=12,
        limit=16,
        scratch=[pltpu.VMEM((2, 16 * PART, 128), F32)],
    )(core, norm1_gain, *state, wt, ra, ca, rb, cb)
    got = lax.ppermute(send, "core", [(0, 1), (1, 0)])
    joined = call(join_kernel, near((16, PART + SLOT, 128), BF16), near=4)(own, got, tab, twin)
    arrived = lax.all_to_all(joined, "lon", split_axis=0, concat_axis=0, tiled=True)
    both, ends = call(
        place_kernel, [near((2, 576, C), BF16), near((2, 192, C), BF16)], near=3
    )(block, slope, back)
    home = lax.ppermute(ends, "lon", [(k, (k + 1) % 16) for k in range(16)])
    part, tab_copies = call(
        lon_sum_kernel, [near((8, PART, 128), BF16), near((16, SLOT, 128), BF16)], near=1
    )(arrived)
    bands = lax.all_to_all(part, ("y", "ens"), split_axis=0, concat_axis=0, tiled=True)
    tab_all = lax.all_to_all(tab_copies, "lon", split_axis=0, concat_axis=0, tiled=True)
    half = call(band_sum_kernel, near((PART, 128), BF16), near=1)(bands)
    other = lax.ppermute(half, "core", [(0, 1), (1, 0)])
    qw, pw, f1, f2, qb, pb, f1b, f2b, n1g, n1o, n2g, n2o = call(
        weight_kernel,
        [shape((36, C), F32), shape((12, C), F32), shape((48, C), F32), shape((12, FF), F32),
         shape((36,), F32), shape((12,), F32), shape((48,), F32)] + [shape((12,), F32)] * 5,
        smem=1,
        near=2,
        scratch=[pltpu.VMEM((2, PART, 128), F32)],
    )(core, half, other)
    tab_out = call(table_kernel, shape((12 * ROWS, 23), F32), near=1)(
        tab_all.reshape(16 * SLOT, 128)
    )
    full = both.reshape(2, *grid[1:])
    ends = home.reshape(2, grid[1], grid[2], 8, C)[:, :, :, :6]
    full = jnp.concatenate([ends, full[:, :, :, 6:]], axis=3)
    return (full[0][None], full[1][None], qw.T, qb, pw.T, pb, f1.T, f1b, f2.T, f2b, n1g, n1o, n2g, n2o,
            tab_out.reshape(bias_table.shape))


def solution(mesh):
    split = Mesh(mesh.devices.reshape(16, 4, 2, 2), ("lon", "y", "core", "ens"))
    lat = ("y", "core")
    tokens = P("ens", None, lat, "lon", None)
    table = P(None, lat, None, None, None, None)
    return jax.shard_map(
        on_device,
        mesh=split,
        in_specs=(tokens, tokens, P(), P(), P(), P(), table) + (P(),) * 8,
        out_specs=(tokens, tokens, P(None, "lon"), P("lon"), P(None, "lon"), P("lon"), P(None, "lon"),
                   P("lon"), P(None, "lon"), P("lon"), P("lon"), P("lon"), P("lon"), P("lon"), table),
        check_vma=False,
    )
```

```python
import math

import jax
import jax.numpy as jnp
from jax import lax
from jax.experimental import pallas as pl
from jax.experimental.pallas import tpu as pltpu
from jax.sharding import Mesh
from jax.sharding import PartitionSpec as P

C = 192
HEADS = 6
FF = 768
ROWS = 144
LANES = 896
HX = 72
TAB = 384
EPS = 1e-05
SCALE = 32 ** -0.5
F32 = jnp.float32
BF16 = jnp.bfloat16
FACTOR = 1.0 / math.sqrt(147456)
GELU_A = 0.044715
GELU_C = math.sqrt(2.0 / math.pi)
PART = 112
SLOT = 32


def nn(a, b):
    return lax.dot_general(a, b, (((1,), (0,)), ((), ())), preferred_element_type=F32)


def nt(a, b):
    return lax.dot_general(a, b, (((1,), (1,)), ((), ())), preferred_element_type=F32)


def tn(a, b):
    return lax.dot_general(a, b, (((0,), (0,)), ((), ())), preferred_element_type=F32)


def iota(dims, axis):
    return lax.broadcasted_iota(jnp.int32, dims, axis).astype(F32)


def whole(value, size):
    return jnp.floor((value + 0.5) * (1.0 / size))


def one_hot(hit):
    return jnp.where(hit, 1.0, 0.0).astype(BF16)


def prep_kernel(qkv_hbm, proj_hbm, fc1_hbm, fc2_hbm, tab_hbm,
                wt_ref, projb_ref, fc1b_ref, fc2b_ref, bias_ref, spread_ref, mask_ref, sel_ref,
                ra_ref, ca_ref, rb_ref, cb_ref, picks_ref, back_ref,
                qkv_ref, proj_ref, fc1_ref, fc2_ref, tab_ref, sems):
    copies = [
        pltpu.make_async_copy(src, dst, sems.at[k])
        for k, (src, dst) in enumerate(
            ((tab_hbm, tab_ref), (qkv_hbm, qkv_ref), (proj_hbm, proj_ref), (fc1_hbm, fc1_ref),
             (fc2_hbm, fc2_ref))
        )
    ]
    for copy in copies:
        copy.start()
    lane = iota((8, LANES), 1)
    cell = whole(lane, HX)
    rest = lane - HX * cell
    head = whole(rest, 12)
    token = 12.0 * (rest - 12.0 * head) + cell
    token = jnp.where(lane < 12.0 * HX, token, -1.0)[0:1]
    head = jnp.where(lane < 12.0 * HX, head, -1.0)[0:1]
    spread_ref[...] = one_hot(iota((ROWS, LANES), 0) == token)
    for h in range(HEADS):
        mask_ref[32 * h : 32 * h + 32, :] = one_hot(
            jnp.broadcast_to(head, (32, LANES)) == float(h)
        )
    row = iota((ROWS, 128), 0)
    level = whole(row, 12)
    base = 44.0 * level - row + 11.0
    column_id = iota((ROWS, 128), 1)
    for i in range(12):
        for t in range(3):
            sel_ref[ROWS * i : ROWS * i + ROWS, 128 * t : 128 * t + 128] = one_hot(
                base + float(i) == column_id + 128.0 * t
            )
    n = iota((576, 128), 0)
    spot = iota((576, 128), 1)
    ca_ref[0:576, :] = one_hot(spot == n - 36.0 * whole(n, 36))
    n = iota((768, 128), 0)
    spot = iota((768, 128), 1)
    ca_ref[576:1344, :] = one_hot(spot == n - 48.0 * whole(n, 48) + 36.0)
    n = iota((192, 128), 0)
    spot = iota((192, 128), 1)
    n = n - 12.0 * whole(n, 12)
    for k in range(6):
        cb_ref[192 * k : 192 * k + 192, :] = one_hot(spot == n + 12.0 * k)
    n = iota((16, 1344), 1)
    n = jnp.where(n < 576.0, whole(n, 36), whole(n - 576.0, 48))
    ra_ref[...] = one_hot(n == iota((16, 1344), 0))
    n = iota((16, 1152), 1)
    n = whole(n - 192.0 * whole(n, 192), 12)
    rb_ref[...] = one_hot(n == iota((16, 1152), 0))
    picks_ref[...] = window_picks()
    back_ref[...] = natural_picks()
    copies[0].wait()
    tiles = []
    for t in range(3):
        tile = None
        for k in range(4):
            piece = tab_ref[pl.ds(4 * t + k, ROWS, stride=12), :]
            piece = jnp.concatenate([piece, jnp.zeros((ROWS, 105), F32)], axis=1)
            if k:
                piece = pltpu.roll(piece, 32 * k, 1)
            tile = piece if tile is None else tile + piece
        tiles.append(tile)
    table = jnp.concatenate(tiles, axis=1)
    high = table.astype(BF16)
    low = (table - high.astype(F32)).astype(BF16)
    pieces = [[], []]
    for i in range(12):
        sel = sel_ref[ROWS * i : ROWS * i + ROWS, :]
        got = nt(sel, high) + nt(sel, low)
        pieces[0].append(got[:, :HX])
        pieces[1].append(got[:, HX:])
    for v in range(2):
        spare = jnp.zeros((ROWS, LANES - 12 * HX), F32)
        bias_ref[v] = jnp.concatenate(pieces[v] + [spare], axis=1)
    copies[1].wait()
    wt_ref[...] = qkv_ref[...].T.astype(BF16)
    copies[2].wait()
    projb_ref[...] = proj_ref[...].astype(BF16)
    copies[3].wait()
    fc1b_ref[...] = fc1_ref[...].astype(BF16)
    copies[4].wait()
    fc2b_ref[...] = fc2_ref[...].astype(BF16)


def column(row):
    size = row.shape[1]
    eye = lax.broadcasted_iota(jnp.int32, (size, size), 0) == lax.broadcasted_iota(
        jnp.int32, (size, size), 1
    )
    return jnp.sum(jnp.where(eye, row, 0.0), axis=1, keepdims=True)


def window_picks():
    r = lax.broadcasted_iota(jnp.int32, (576, 128), 0).astype(F32)
    m = jnp.floor((r + 0.5) * (1.0 / 12.0))
    j = r - 12.0 * m
    second = m >= 24.0
    n = jnp.where(second, m - 24.0, m)
    src = jnp.where(second, 24.0 * n + 18.0 + j, 24.0 * n + 6.0 + j)
    src = jnp.where(second & (j >= 6.0), 570.0 + 8.0 * n + j, src)
    lane = lax.broadcasted_iota(jnp.int32, (576, 128), 1).astype(F32)
    tiles = [jnp.where(src == lane + 128.0 * t, 1.0, 0.0).astype(BF16) for t in range(6)]
    return jnp.concatenate(tiles, axis=1)


def natural_picks():
    p = lax.broadcasted_iota(jnp.int32, (768, 128), 0).astype(F32)
    own = p < 576.0
    q = p - 576.0
    n = jnp.where(own, jnp.floor((p + 0.5) * (1.0 / 24.0)), jnp.floor((q + 0.5) * 0.125))
    c = jnp.where(own, p - 24.0 * n, q - 8.0 * n)
    inner = jnp.where(c < 18.0, 12.0 * n + c - 6.0, 288.0 + 12.0 * n + c - 18.0)
    inner = jnp.where(c < 6.0, -1.0, inner)
    outer = jnp.where(c < 6.0, 294.0 + 12.0 * n + c, -1.0)
    dst = jnp.where(own, inner, outer)
    lane = lax.broadcasted_iota(jnp.int32, (768, 128), 1).astype(F32)
    tiles = [jnp.where(dst == lane + 128.0 * t, 1.0, 0.0).astype(BF16) for t in range(5)]
    return jnp.concatenate(tiles, axis=1)[:, :576]


def norm_parts(values):
    centre = jnp.sum(values, axis=1, keepdims=True) * (1.0 / C)
    centred = values - centre
    spread = jnp.sum(centred * centred, axis=1, keepdims=True) * (1.0 / C)
    inverse = lax.rsqrt(spread + EPS)
    return centred * inverse, inverse


def norm_back(grad, hat, inverse, gain):
    scaled = grad * gain
    first = jnp.sum(scaled, axis=1, keepdims=True) * (1.0 / C)
    second = jnp.sum(scaled * hat, axis=1, keepdims=True) * (1.0 / C)
    return inverse * (scaled - first - hat * second)


def front_kernel(x_ref, cot_ref, n1g_ref, n1o_ref, qb_ref, pb_ref, n2g_ref, n2o_ref,
                 f1b_ref, f2b_ref, halo_ref, bias_ref, wt_ref, proj_ref, fc1_ref, fc2_ref,
                 spread_ref, mask_ref, sel_ref, picks_ref,
                 low_ref, block_ref, few_ref, wide_ref, hat_ref, inv_ref, rg_ref, row_ref, f1s_ref,
                 sum_ref, tab_ref):
    n1g, n1o, qb, pb, n2g, n2o, f1b, f2b = (
        ref[...].reshape(1, -1)
        for ref in (n1g_ref, n1o_ref, qb_ref, pb_ref, n2g_ref, n2o_ref, f1b_ref, f2b_ref)
    )
    picks = picks_ref[...]
    xw = nn(picks, jnp.concatenate([x_ref[...], halo_ref[0]], axis=0))
    cw = nn(picks, jnp.concatenate([cot_ref[...], halo_ref[1]], axis=0))
    cot_low = cw.astype(BF16)
    hat1, inv1 = norm_parts(xw)
    normed = (hat1 * n1g + n1o).astype(BF16)
    wq = wt_ref[0:192, :]
    wk = wt_ref[192:384, :]
    wv = wt_ref[384:576, :]
    bq_row = qb[:, 0:192]
    bk_row = qb[:, 192:384]
    bv_row = qb[:, 384:576]
    bq = column(bq_row)
    bk = column(bk_row)
    bv = column(bv_row)
    keys = (nt(normed, wk) + bk_row).astype(BF16)
    values = (nt(normed, wv) + bv_row).astype(BF16)
    spread = spread_ref[...]
    mask = mask_ref[...]
    saved = []
    attended = []
    for g in range(4):
        rows = slice(ROWS * g, ROWS * g + ROWS)
        own = normed[rows]
        query_t = (nt(wq, own) + bq).astype(BF16)
        value_t = (nt(wv, own) + bv).astype(BF16)
        query_bd = nn(query_t, spread).astype(BF16) * mask
        scores = nn(keys[rows], query_bd) * SCALE + bias_ref[g % 2]
        peak = jnp.max(scores, axis=0, keepdims=True)
        raised = jnp.exp(scores - peak)
        total = jnp.sum(raised, axis=0, keepdims=True)
        weights = (raised * (1.0 / total)).astype(BF16)
        mixed = nn(value_t, weights).astype(BF16) * mask
        attended.append(nt(spread, mixed).astype(BF16))
        saved.append((query_bd, weights))
    attended = jnp.concatenate(attended, axis=0)
    attn_out = (nn(attended, proj_ref[...]) + pb).astype(BF16)
    resid = xw + attn_out.astype(F32)
    hat2, inv2 = norm_parts(resid)
    normed2 = (hat2 * n2g + n2o).astype(BF16)
    acts = []
    grads = []
    f1_sums = []
    for g in range(4):
        rows = slice(ROWS * g, ROWS * g + ROWS)
        u = nn(normed2[rows], fc1_ref[...]) + f1b
        square = u * u
        half = 0.5 * jnp.tanh(u * (GELU_C + (GELU_A * GELU_C) * square)) + 0.5
        acts.append((u * half).astype(BF16))
        lean = u * (2.0 * GELU_C + (6.0 * GELU_A * GELU_C) * square)
        slope = half + (half - half * half) * lean
        act_grad = nn(cot_low[rows], fc2_ref[...])
        pre = (act_grad * slope).astype(BF16)
        grads.append(pre)
        f1_sums.append(jnp.sum(pre.astype(F32), axis=0, keepdims=True))
    activated = jnp.concatenate(acts, axis=0)
    pre_grad = jnp.concatenate(grads, axis=0)
    f1_sum = f1_sums[0] + f1_sums[1] + f1_sums[2] + f1_sums[3]
    block = (resid + nt(activated, fc2_ref[...]) + f2b).astype(BF16)
    block_ref[...] = block
    n2_grad = nt(pre_grad, fc1_ref[...])
    n2g_sum = jnp.sum(n2_grad * hat2, axis=0, keepdims=True)
    n2o_sum = jnp.sum(n2_grad, axis=0, keepdims=True)
    resid_grad = cw + norm_back(n2_grad, hat2, inv2, n2g)
    attn_grad = resid_grad.astype(BF16)
    pb_sum = jnp.sum(attn_grad.astype(F32), axis=0, keepdims=True)
    f2_sum = jnp.sum(cw, axis=0, keepdims=True)
    grad_q = []
    grad_k = []
    grad_v = []
    for g in range(4):
        rows = slice(ROWS * g, ROWS * g + ROWS)
        query_bd, weights = saved[g]
        own = normed[rows]
        grad_t = nt(proj_ref[...], attn_grad[rows]).astype(BF16)
        grad_bd = nn(grad_t, spread).astype(BF16) * mask
        prob_grad = nn(values[rows], grad_bd)
        probs = weights.astype(F32)
        shared = jnp.sum(probs * prob_grad, axis=0, keepdims=True)
        score_grad = probs * (prob_grad - shared)
        if g < 2:
            sum_ref[g] = score_grad
        else:
            sum_ref[g - 2] += score_grad
        low = score_grad.astype(BF16)
        grad_v.append(nt(weights, grad_bd).astype(BF16))
        grad_k.append((nt(low, query_bd) * SCALE).astype(BF16))
        key_t = (nt(wk, own) + bk).astype(BF16)
        mixed = (nn(key_t, low) * SCALE).astype(BF16) * mask
        grad_q.append(nt(spread, mixed).astype(BF16))
    for v in range(2):
        turned = sum_ref[v].T
        total = jnp.zeros((HX, TAB), F32)
        for i in range(12):
            piece = turned[HX * i : HX * i + HX, :].astype(BF16)
            total = total + nn(piece, sel_ref[ROWS * i : ROWS * i + ROWS, :])
        for t in range(3):
            tab_ref[ROWS * t + HX * v : ROWS * t + HX * v + HX, :] = total[:, 128 * t : 128 * t + 128]
    tab_ref[3 * ROWS :, :] = jnp.zeros((16 * SLOT - 3 * ROWS, 128), F32)
    for l in range(16):
        low_ref[l] = tab_ref[SLOT * l : SLOT * l + SLOT, :].astype(BF16)
    for k, group in enumerate((grad_q, grad_k, grad_v)):
        for g in range(4):
            few_ref[k, ROWS * g : ROWS * g + ROWS, :] = group[g]
    few_ref[3] = normed
    few_ref[4] = normed2
    few_ref[5] = cot_low
    few_ref[6] = attn_grad
    few_ref[7] = attended
    wide_ref[0] = pre_grad
    wide_ref[1] = activated
    hat_ref[...] = hat1
    inv_ref[...] = inv1
    rg_ref[...] = resid_grad
    row_ref[0:1, :] = pb_sum
    row_ref[1:2, :] = f2_sum
    row_ref[2:3, :] = n2g_sum
    row_ref[3:4, :] = n2o_sum
    f1s_ref[...] = f1_sum


def back_kernel(core_ref, n1g_ref, few_ref, wide_ref, hat_ref, inv_ref, rg_ref, row_ref,
                f1s_ref, wt_ref, ra_ref, ca_ref, rb_ref, cb_ref, low_ref,
                ig_ref, own_ref, send_ref, tab_ref, stage_ref):
    tab_ref[...] = low_ref[...]
    wq = wt_ref[0:192, :]
    wk = wt_ref[192:384, :]
    wv = wt_ref[384:576, :]
    n1g = n1g_ref[...].reshape(1, -1)
    dq = few_ref[0]
    dk = few_ref[1]
    dv = few_ref[2]
    normed = few_ref[3]
    hat1 = hat_ref[...]
    f1_sum = f1s_ref[...]
    pb_sum = row_ref[0:1, :]
    f2_sum = row_ref[1:2, :]
    n2g_sum = row_ref[2:3, :]
    n2o_sum = row_ref[3:4, :]
    n1_grad = nn(dq, wq) + nn(dk, wk) + nn(dv, wv)
    n1g_sum = jnp.sum(n1_grad * hat1, axis=0, keepdims=True)
    n1o_sum = jnp.sum(n1_grad, axis=0, keepdims=True)
    input_grad = (rg_ref[...] + norm_back(n1_grad, hat1, inv_ref[...], n1g)).astype(BF16)
    ig_ref[...] = input_grad
    sums = [jnp.sum(d.astype(F32), axis=0, keepdims=True) for d in (dq, dk, dv)]
    dw_q = tn(dq, normed)
    dw_k = tn(dk, normed)
    dw_v = tn(dv, normed)
    dw_qkv = jnp.concatenate([dw_q, dw_k, dw_v], axis=0)
    dw_p = tn(few_ref[6], few_ref[7])
    dw_1 = tn(wide_ref[0], few_ref[4])
    dw_2 = tn(few_ref[5], wide_ref[1])
    vec_a = jnp.concatenate(sums + [f1_sum[:, 0:192], f1_sum[:, 192:384], f1_sum[:, 384:576], f1_sum[:, 576:768]], axis=1)
    vec_b = jnp.concatenate([pb_sum, f2_sum, n1g_sum, n1o_sum, n2g_sum, n2o_sum], axis=1)
    row_a = nn((ra_ref[...].astype(F32) * vec_a).astype(BF16), ca_ref[...])
    row_b = nn((rb_ref[...].astype(F32) * vec_b).astype(BF16), cb_ref[...])
    for l in range(16):
        a36 = dw_qkv[36 * l : 36 * l + 36]
        a12 = dw_p[12 * l : 12 * l + 12]
        b48 = dw_1[48 * l : 48 * l + 48]
        d12 = dw_2[12 * l : 12 * l + 12]
        top = PART * l
        stage_ref[0, top : top + 36, :] = a36[:, :128]
        stage_ref[0, top + 36 : top + 48, :] = a12[:, :128]
        a_rest = jnp.concatenate([a36[:, 128:], a12[:, 128:]], axis=0)
        stage_ref[0, top + 48 : top + 96, :] = jnp.concatenate([a_rest, b48[:, 128:]], axis=1)
        stage_ref[0, top + 96 : top + 108, :] = d12[:, 640:]
        stage_ref[0, top + 108 : top + 109, :] = row_a[l : l + 1]
        stage_ref[0, top + 109 : top + 110, :] = row_b[l : l + 1]
        stage_ref[0, top + 110 : top + 112, :] = jnp.zeros((2, 128), F32)
        stage_ref[1, top : top + 48, :] = b48[:, :128]
        for b in range(5):
            stage_ref[1, top + 48 + 12 * b : top + 60 + 12 * b, :] = d12[:, 128 * b : 128 * b + 128]
        stage_ref[1, top + 108 : top + 112, :] = jnp.zeros((4, 128), F32)
    core = core_ref[0]
    own_ref[...] = stage_ref[core].astype(BF16)
    send_ref[...] = stage_ref[1 - core].astype(BF16)


def place_kernel(block_ref, ig_ref, back_ref, out_ref, edge_ref):
    back = back_ref[...]
    for k, ref in enumerate((block_ref, ig_ref)):
        placed = nn(back, ref[...]).astype(BF16)
        out_ref[k] = placed[:576]
        edge_ref[k] = placed[576:]


def edge_kernel(x_hbm, cot_hbm, out_ref, sems):
    copies = [
        pltpu.make_async_copy(src.at[:, 0:8, :], out_ref.at[k], sems.at[k])
        for k, src in enumerate((x_hbm, cot_hbm))
    ]
    for copy in copies:
        copy.start()
    for copy in copies:
        copy.wait()


def join_kernel(own_ref, got_ref, tab_ref, out_ref):
    table = tab_ref[0].astype(F32)
    for l in range(1, 16):
        table = table + tab_ref[l].astype(F32)
    low = table.astype(BF16)
    for l in range(16):
        part = slice(PART * l, PART * l + PART)
        out_ref[l, 0:PART, :] = (own_ref[part].astype(F32) + got_ref[part].astype(F32)).astype(BF16)
        out_ref[l, PART:, :] = low


def lon_sum_kernel(in_ref, part_ref, tab_ref):
    total = in_ref[0, 0:PART].astype(F32)
    for l in range(1, 16):
        total = total + in_ref[l, 0:PART].astype(F32)
    low = total.astype(BF16)
    for k in range(8):
        part_ref[k] = low
    for l in range(16):
        tab_ref[SLOT * l : SLOT * l + SLOT, :] = in_ref[l, PART:]


def band_sum_kernel(in_ref, out_ref):
    total = in_ref[0].astype(F32)
    for k in range(1, 8):
        total = total + in_ref[k].astype(F32)
    out_ref[...] = total.astype(BF16)


def weight_kernel(core_ref, own_ref, got_ref, qw_ref, pw_ref, f1_ref, f2_ref, qb_ref, pb_ref, f1b_ref,
                  f2b_ref, n1g_ref, n1o_ref, n2g_ref, n2o_ref, pair_ref):
    core = core_ref[0]
    pair_ref[core] = own_ref[...].astype(F32) * FACTOR
    pair_ref[1 - core] = got_ref[...].astype(F32) * FACTOR
    first = pair_ref[0]
    second = pair_ref[1]
    a = jnp.concatenate([first[0:48], first[48:96, 0:64]], axis=1)
    qw_ref[...] = a[0:36]
    pw_ref[...] = a[36:48]
    f1_ref[...] = jnp.concatenate([second[0:48], first[48:96, 64:128]], axis=1)
    d = [second[48 + 12 * k : 60 + 12 * k] for k in range(5)] + [first[96:108]]
    f2_ref[...] = jnp.concatenate(d, axis=1)
    va = first[108:109]
    vb = first[109:110]
    qb_ref[...] = va[:, 0:36].reshape(36)
    f1b_ref[...] = va[:, 36:84].reshape(48)
    for k, ref in enumerate((pb_ref, f2b_ref, n1g_ref, n1o_ref, n2g_ref, n2o_ref)):
        ref[...] = vb[:, 12 * k : 12 * k + 12].reshape(12)


def table_kernel(tab_ref, twin_ref, out_tab_ref):
    tab = tab_ref[...].astype(F32) + twin_ref[...].astype(F32)
    for t in range(3):
        tile = tab[ROWS * t : ROWS * t + ROWS]
        for k in range(4):
            piece = pltpu.roll(tile, 128 - 32 * k, 1) if k else tile
            out_tab_ref[pl.ds(4 * t + k, ROWS, stride=12), :] = piece[:, :23]


def call(kernel, out_shape, smem=0, far=0, near=0, limit=8, scratch=(), raw=False, flops=0):
    count = smem + far + near
    space = pltpu.HBM if raw else pltpu.VMEM
    specs = [pl.BlockSpec(memory_space=pltpu.SMEM)] * smem + [
        pl.BlockSpec(memory_space=space)
    ] * (far + near)
    run = pl.pallas_call(
        kernel,
        out_shape=out_shape,
        in_specs=specs,
        out_specs=jax.tree.map(lambda _: pl.BlockSpec(memory_space=pltpu.VMEM), out_shape),
        scratch_shapes=scratch,
        compiler_params=pltpu.CompilerParams(vmem_limit_bytes=limit << 20),
        cost_estimate=pl.CostEstimate(flops=flops, transcendentals=0, bytes_accessed=0)
        if flops
        else None,
    )

    def go(*args):
        if raw:
            args = tuple(pltpu.with_memory_space_constraint(a, pltpu.HBM) for a in args)
        kept = args[: smem + far] + tuple(
            pltpu.with_memory_space_constraint(a, pltpu.VMEM) for a in args[smem + far :]
        )
        assert len(args) == count
        return run(*kept)

    return go


def near(dims, dtype):
    return pltpu.VMEM(dims, dtype)


def shape(dims, dtype):
    return jax.ShapeDtypeStruct(dims, dtype)


def on_device(inputs, cotangent, norm1_gain, norm1_offset, qkv_weight, qkv_bias, bias_table,
              proj_weight, proj_bias, norm2_gain, norm2_offset, fc1_weight, fc1_bias,
              fc2_weight, fc2_bias):
    grid = inputs.shape
    x = inputs.reshape(576, C)
    cot = cotangent.reshape(576, C)
    edge = call(
        edge_kernel, near((2, 24, 8, C), BF16), far=2, raw=True,
        scratch=[pltpu.SemaphoreType.DMA((2,))],
    )(inputs.reshape(24, 24, C), cotangent.reshape(24, 24, C)).reshape(2, 192, C)
    halo = lax.ppermute(edge, "lon", [(k, (k - 1) % 16) for k in range(16)])
    table = bias_table.reshape(12 * ROWS, 23)
    wt, proj, fc1, fc2, bias, spread, mask, sel, ra, ca, rb, cb, picks, back = call(
        prep_kernel,
        [near((576, C), BF16), near((C, C), BF16), near((C, FF), BF16), near((C, FF), BF16),
         near((2, ROWS, LANES), F32), near((ROWS, LANES), BF16), near((C, LANES), BF16),
         near((12 * ROWS, TAB), BF16), near((16, 1344), BF16), near((1344, 128), BF16),
         near((16, 1152), BF16), near((1152, 128), BF16), near((576, 768), BF16), near((768, 576), BF16)],
        far=5,
        limit=16,
        raw=True,
        scratch=[pltpu.VMEM((C, 576), F32), pltpu.VMEM((C, C), F32), pltpu.VMEM((C, FF), F32),
                 pltpu.VMEM((C, FF), F32), pltpu.VMEM((12 * ROWS, 23), F32),
                 pltpu.SemaphoreType.DMA((5,))],
    )(qkv_weight, proj_weight, fc1_weight, fc2_weight.T, table)
    core = lax.axis_index("core").astype(jnp.int32).reshape(1)
    tab, block, *state = call(
        front_kernel,
        [near((16, SLOT, 128), BF16), near((576, C), BF16), near((8, 576, C), BF16),
         near((2, 576, FF), BF16), near((576, C), F32), near((576, 1), F32), near((576, C), F32),
         near((8, C), F32), near((1, FF), F32)],
        far=10,
        near=10,
        limit=24,
        scratch=[pltpu.VMEM((2, ROWS, LANES), F32), pltpu.VMEM((16 * SLOT, 128), F32)],
    )(x, cot, norm1_gain, norm1_offset, qkv_bias, proj_bias, norm2_gain, norm2_offset, fc1_bias,
      fc2_bias, halo, bias, wt, proj, fc1, fc2, spread, mask, sel, picks)
    slope, own, send, tab = call(
        back_kernel,
        [near((576, C), BF16), near((16 * PART, 128), BF16), near((16 * PART, 128), BF16),
         shape((16, SLOT, 128), BF16)],
        smem=1,
        far=1,
        near=13,
        limit=16,
        scratch=[pltpu.VMEM((2, 16 * PART, 128), F32)],
    )(core, norm1_gain, *state, wt, ra, ca, rb, cb, tab)
    tab = lax.all_to_all(tab, "lon", split_axis=0, concat_axis=0, tiled=True)
    got = lax.ppermute(send, "core", [(0, 1), (1, 0)])
    joined = call(join_kernel, near((16, PART + SLOT, 128), BF16), near=3)(own, got, tab)
    arrived = lax.all_to_all(joined, "lon", split_axis=0, concat_axis=0, tiled=True)
    both, ends = call(
        place_kernel, [near((2, 576, C), BF16), near((2, 192, C), BF16)], near=3
    )(block, slope, back)
    home = lax.ppermute(ends, "lon", [(k, (k + 1) % 16) for k in range(16)])
    part, tab_all = call(
        lon_sum_kernel, [near((8, PART, 128), BF16), near((16 * SLOT, 128), BF16)], near=1
    )(arrived)
    bands = lax.all_to_all(part, ("y", "ens"), split_axis=0, concat_axis=0, tiled=True)
    twin = lax.ppermute(tab_all, "ens", [(0, 1), (1, 0)])
    half = call(band_sum_kernel, near((PART, 128), BF16), near=1)(bands)
    other = lax.ppermute(half, "core", [(0, 1), (1, 0)])
    qw, pw, f1, f2, qb, pb, f1b, f2b, n1g, n1o, n2g, n2o = call(
        weight_kernel,
        [shape((36, C), F32), shape((12, C), F32), shape((48, C), F32), shape((12, FF), F32),
         shape((36,), F32), shape((12,), F32), shape((48,), F32)] + [shape((12,), F32)] * 5,
        smem=1,
        near=2,
        scratch=[pltpu.VMEM((2, PART, 128), F32)],
    )(core, half, other)
    tab_out = call(table_kernel, shape((12 * ROWS, 23), F32), near=2)(tab_all, twin)
    full = both.reshape(2, *grid[1:])
    ends = home.reshape(2, grid[1], grid[2], 8, C)[:, :, :, :6]
    full = jnp.concatenate([ends, full[:, :, :, 6:]], axis=3)
    return (full[0][None], full[1][None], qw.T, qb, pw.T, pb, f1.T, f1b, f2.T, f2b, n1g, n1o, n2g, n2o,
            tab_out.reshape(bias_table.shape))


def solution(mesh):
    split = Mesh(mesh.devices.reshape(16, 4, 2, 2), ("lon", "y", "core", "ens"))
    lat = ("y", "core")
    tokens = P("ens", None, lat, "lon", None)
    table = P(None, lat, None, None, None, None)
    return jax.shard_map(
        on_device,
        mesh=split,
        in_specs=(tokens, tokens, P(), P(), P(), P(), table) + (P(),) * 8,
        out_specs=(tokens, tokens, P(None, "lon"), P("lon"), P(None, "lon"), P("lon"), P(None, "lon"),
                   P("lon"), P(None, "lon"), P("lon"), P("lon"), P("lon"), P("lon"), P("lon"), table),
        check_vma=False,
    )
```

```python
import math

import jax
import jax.numpy as jnp
from jax import lax
from jax.experimental import pallas as pl
from jax.experimental.pallas import tpu as pltpu
from jax.sharding import Mesh
from jax.sharding import PartitionSpec as P

C = 192
HEADS = 6
FF = 768
ROWS = 144
LANES = 896
HX = 72
TAB = 384
EPS = 1e-05
SCALE = 32 ** -0.5
F32 = jnp.float32
BF16 = jnp.bfloat16
FACTOR = 1.0 / math.sqrt(147456)
GELU_A = 0.044715
GELU_C = math.sqrt(2.0 / math.pi)
PART = 112
SLOT = 32


def nn(a, b):
    return lax.dot_general(a, b, (((1,), (0,)), ((), ())), preferred_element_type=F32)


def nt(a, b):
    return lax.dot_general(a, b, (((1,), (1,)), ((), ())), preferred_element_type=F32)


def tn(a, b):
    return lax.dot_general(a, b, (((0,), (0,)), ((), ())), preferred_element_type=F32)


def iota(dims, axis):
    return lax.broadcasted_iota(jnp.int32, dims, axis).astype(F32)


def whole(value, size):
    return jnp.floor((value + 0.5) * (1.0 / size))


def one_hot(hit):
    return jnp.where(hit, 1.0, 0.0).astype(BF16)


def prep_kernel(qkv_hbm, proj_hbm, fc1_hbm, fc2_hbm, tab_hbm,
                wt_ref, projb_ref, fc1b_ref, fc2b_ref, bias_ref, spread_ref, mask_ref, sel_ref,
                ra_ref, ca_ref, rb_ref, cb_ref, picks_ref, back_ref,
                qkv_ref, proj_ref, fc1_ref, fc2_ref, tab_ref, sems):
    copies = [
        pltpu.make_async_copy(src, dst, sems.at[k])
        for k, (src, dst) in enumerate(
            ((tab_hbm, tab_ref), (qkv_hbm, qkv_ref), (proj_hbm, proj_ref), (fc1_hbm, fc1_ref),
             (fc2_hbm, fc2_ref))
        )
    ]
    for copy in copies:
        copy.start()
    lane = iota((8, LANES), 1)
    cell = whole(lane, HX)
    rest = lane - HX * cell
    head = whole(rest, 12)
    token = 12.0 * (rest - 12.0 * head) + cell
    token = jnp.where(lane < 12.0 * HX, token, -1.0)[0:1]
    head = jnp.where(lane < 12.0 * HX, head, -1.0)[0:1]
    spread_ref[...] = one_hot(iota((ROWS, LANES), 0) == token)
    for h in range(HEADS):
        mask_ref[32 * h : 32 * h + 32, :] = one_hot(
            jnp.broadcast_to(head, (32, LANES)) == float(h)
        )
    row = iota((ROWS, 128), 0)
    level = whole(row, 12)
    base = 44.0 * level - row + 11.0
    column_id = iota((ROWS, 128), 1)
    for i in range(12):
        for t in range(3):
            sel_ref[ROWS * i : ROWS * i + ROWS, 128 * t : 128 * t + 128] = one_hot(
                base + float(i) == column_id + 128.0 * t
            )
    n = iota((576, 128), 0)
    spot = iota((576, 128), 1)
    ca_ref[0:576, :] = one_hot(spot == n - 36.0 * whole(n, 36))
    n = iota((768, 128), 0)
    spot = iota((768, 128), 1)
    ca_ref[576:1344, :] = one_hot(spot == n - 48.0 * whole(n, 48) + 36.0)
    n = iota((192, 128), 0)
    spot = iota((192, 128), 1)
    n = n - 12.0 * whole(n, 12)
    for k in range(6):
        cb_ref[192 * k : 192 * k + 192, :] = one_hot(spot == n + 12.0 * k)
    n = iota((16, 1344), 1)
    n = jnp.where(n < 576.0, whole(n, 36), whole(n - 576.0, 48))
    ra_ref[...] = one_hot(n == iota((16, 1344), 0))
    n = iota((16, 1152), 1)
    n = whole(n - 192.0 * whole(n, 192), 12)
    rb_ref[...] = one_hot(n == iota((16, 1152), 0))
    picks_ref[...] = window_picks()
    back_ref[...] = natural_picks()
    copies[0].wait()
    tiles = []
    for t in range(3):
        tile = None
        for k in range(4):
            piece = tab_ref[pl.ds(4 * t + k, ROWS, stride=12), :]
            piece = jnp.concatenate([piece, jnp.zeros((ROWS, 105), F32)], axis=1)
            if k:
                piece = pltpu.roll(piece, 32 * k, 1)
            tile = piece if tile is None else tile + piece
        tiles.append(tile)
    table = jnp.concatenate(tiles, axis=1)
    high = table.astype(BF16)
    low = (table - high.astype(F32)).astype(BF16)
    pieces = [[], []]
    for i in range(12):
        sel = sel_ref[ROWS * i : ROWS * i + ROWS, :]
        got = nt(sel, high) + nt(sel, low)
        pieces[0].append(got[:, :HX])
        pieces[1].append(got[:, HX:])
    for v in range(2):
        spare = jnp.zeros((ROWS, LANES - 12 * HX), F32)
        bias_ref[v] = jnp.concatenate(pieces[v] + [spare], axis=1)
    copies[1].wait()
    wt_ref[...] = qkv_ref[...].T.astype(BF16)
    copies[2].wait()
    projb_ref[...] = proj_ref[...].astype(BF16)
    copies[3].wait()
    fc1b_ref[...] = fc1_ref[...].astype(BF16)
    copies[4].wait()
    fc2b_ref[...] = fc2_ref[...].astype(BF16)


def column(row):
    size = row.shape[1]
    eye = lax.broadcasted_iota(jnp.int32, (size, size), 0) == lax.broadcasted_iota(
        jnp.int32, (size, size), 1
    )
    return jnp.sum(jnp.where(eye, row, 0.0), axis=1, keepdims=True)


def window_picks():
    r = lax.broadcasted_iota(jnp.int32, (576, 128), 0).astype(F32)
    m = jnp.floor((r + 0.5) * (1.0 / 12.0))
    j = r - 12.0 * m
    second = m >= 24.0
    n = jnp.where(second, m - 24.0, m)
    src = jnp.where(second, 24.0 * n + 18.0 + j, 24.0 * n + 6.0 + j)
    src = jnp.where(second & (j >= 6.0), 570.0 + 8.0 * n + j, src)
    lane = lax.broadcasted_iota(jnp.int32, (576, 128), 1).astype(F32)
    tiles = [jnp.where(src == lane + 128.0 * t, 1.0, 0.0).astype(BF16) for t in range(6)]
    return jnp.concatenate(tiles, axis=1)


def natural_picks():
    p = lax.broadcasted_iota(jnp.int32, (768, 128), 0).astype(F32)
    own = p < 576.0
    q = p - 576.0
    n = jnp.where(own, jnp.floor((p + 0.5) * (1.0 / 24.0)), jnp.floor((q + 0.5) * 0.125))
    c = jnp.where(own, p - 24.0 * n, q - 8.0 * n)
    inner = jnp.where(c < 18.0, 12.0 * n + c - 6.0, 288.0 + 12.0 * n + c - 18.0)
    inner = jnp.where(c < 6.0, -1.0, inner)
    outer = jnp.where(c < 6.0, 294.0 + 12.0 * n + c, -1.0)
    dst = jnp.where(own, inner, outer)
    lane = lax.broadcasted_iota(jnp.int32, (768, 128), 1).astype(F32)
    tiles = [jnp.where(dst == lane + 128.0 * t, 1.0, 0.0).astype(BF16) for t in range(5)]
    return jnp.concatenate(tiles, axis=1)[:, :576]


def norm_parts(values):
    centre = jnp.sum(values, axis=1, keepdims=True) * (1.0 / C)
    centred = values - centre
    spread = jnp.sum(centred * centred, axis=1, keepdims=True) * (1.0 / C)
    inverse = lax.rsqrt(spread + EPS)
    return centred * inverse, inverse


def norm_back(grad, hat, inverse, gain):
    scaled = grad * gain
    first = jnp.sum(scaled, axis=1, keepdims=True) * (1.0 / C)
    second = jnp.sum(scaled * hat, axis=1, keepdims=True) * (1.0 / C)
    return inverse * (scaled - first - hat * second)


def front_kernel(x_ref, cot_ref, n1g_ref, n1o_ref, qb_ref, pb_ref, n2g_ref, n2o_ref,
                 f1b_ref, f2b_ref, halo_ref, bias_ref, wt_ref, proj_ref, fc1_ref, fc2_ref,
                 spread_ref, mask_ref, sel_ref, picks_ref,
                 low_ref, block_ref, few_ref, wide_ref, hat_ref, inv_ref, rg_ref, row_ref, f1s_ref,
                 sum_ref, tab_ref):
    n1g, n1o, qb, pb, n2g, n2o, f1b, f2b = (
        ref[...].reshape(1, -1)
        for ref in (n1g_ref, n1o_ref, qb_ref, pb_ref, n2g_ref, n2o_ref, f1b_ref, f2b_ref)
    )
    picks = picks_ref[...]
    xw = nn(picks, jnp.concatenate([x_ref[...], halo_ref[0]], axis=0))
    cw = nn(picks, jnp.concatenate([cot_ref[...], halo_ref[1]], axis=0))
    cot_low = cw.astype(BF16)
    hat1, inv1 = norm_parts(xw)
    normed = (hat1 * n1g + n1o).astype(BF16)
    wq = wt_ref[0:192, :]
    wk = wt_ref[192:384, :]
    wv = wt_ref[384:576, :]
    bq_row = qb[:, 0:192]
    bk_row = qb[:, 192:384]
    bv_row = qb[:, 384:576]
    bq = column(bq_row)
    bk = column(bk_row)
    bv = column(bv_row)
    keys = (nt(normed, wk) + bk_row).astype(BF16)
    values = (nt(normed, wv) + bv_row).astype(BF16)
    spread = spread_ref[...]
    mask = mask_ref[...]
    saved = []
    attended = []

    def begin(g):
        own = normed[ROWS * g : ROWS * g + ROWS]
        query_t = (nt(wq, own) + bq).astype(BF16)
        value_t = (nt(wv, own) + bv).astype(BF16)
        query_bd = nn(query_t, spread).astype(BF16) * mask
        return query_bd, value_t, nn(keys[ROWS * g : ROWS * g + ROWS], query_bd)

    ahead = begin(0)
    for g in range(4):
        query_bd, value_t, raw = ahead
        if g < 3:
            ahead = begin(g + 1)
        scores = raw * SCALE + bias_ref[g % 2]
        peak = jnp.max(scores, axis=0, keepdims=True)
        raised = jnp.exp(scores - peak)
        total = jnp.sum(raised, axis=0, keepdims=True)
        weights = (raised * (1.0 / total)).astype(BF16)
        mixed = nn(value_t, weights).astype(BF16) * mask
        attended.append(nt(spread, mixed).astype(BF16))
        saved.append((query_bd, weights))
    attended = jnp.concatenate(attended, axis=0)
    attn_out = (nn(attended, proj_ref[...]) + pb).astype(BF16)
    resid = xw + attn_out.astype(F32)
    hat2, inv2 = norm_parts(resid)
    normed2 = (hat2 * n2g + n2o).astype(BF16)
    acts = []
    grads = []
    f1_sums = []

    def feed(g):
        rows = slice(ROWS * g, ROWS * g + ROWS)
        return nn(normed2[rows], fc1_ref[...]), nn(cot_low[rows], fc2_ref[...])

    ahead = feed(0)
    for g in range(4):
        u, act_grad = ahead
        if g < 3:
            ahead = feed(g + 1)
        u = u + f1b
        square = u * u
        half = 0.5 * jnp.tanh(u * (GELU_C + (GELU_A * GELU_C) * square)) + 0.5
        acts.append((u * half).astype(BF16))
        lean = u * (2.0 * GELU_C + (6.0 * GELU_A * GELU_C) * square)
        slope = half + (half - half * half) * lean
        pre = (act_grad * slope).astype(BF16)
        grads.append(pre)
        f1_sums.append(jnp.sum(pre.astype(F32), axis=0, keepdims=True))
    activated = jnp.concatenate(acts, axis=0)
    pre_grad = jnp.concatenate(grads, axis=0)
    f1_sum = f1_sums[0] + f1_sums[1] + f1_sums[2] + f1_sums[3]
    block = (resid + nt(activated, fc2_ref[...]) + f2b).astype(BF16)
    block_ref[...] = block
    n2_grad = nt(pre_grad, fc1_ref[...])
    n2g_sum = jnp.sum(n2_grad * hat2, axis=0, keepdims=True)
    n2o_sum = jnp.sum(n2_grad, axis=0, keepdims=True)
    resid_grad = cw + norm_back(n2_grad, hat2, inv2, n2g)
    attn_grad = resid_grad.astype(BF16)
    pb_sum = jnp.sum(attn_grad.astype(F32), axis=0, keepdims=True)
    f2_sum = jnp.sum(cw, axis=0, keepdims=True)
    grad_q = []
    grad_k = []
    grad_v = []

    def reach(g):
        rows = slice(ROWS * g, ROWS * g + ROWS)
        grad_t = nt(proj_ref[...], attn_grad[rows]).astype(BF16)
        grad_bd = nn(grad_t, spread).astype(BF16) * mask
        return grad_bd, nn(values[rows], grad_bd)

    ahead = reach(0)
    for g in range(4):
        query_bd, weights = saved[g]
        own = normed[ROWS * g : ROWS * g + ROWS]
        grad_bd, prob_grad = ahead
        if g < 3:
            ahead = reach(g + 1)
        probs = weights.astype(F32)
        shared = jnp.sum(probs * prob_grad, axis=0, keepdims=True)
        score_grad = probs * (prob_grad - shared)
        if g < 2:
            sum_ref[g] = score_grad
        else:
            sum_ref[g - 2] += score_grad
        low = score_grad.astype(BF16)
        grad_v.append(nt(weights, grad_bd).astype(BF16))
        grad_k.append((nt(low, query_bd) * SCALE).astype(BF16))
        key_t = (nt(wk, own) + bk).astype(BF16)
        mixed = (nn(key_t, low) * SCALE).astype(BF16) * mask
        grad_q.append(nt(spread, mixed).astype(BF16))
    for v in range(2):
        turned = sum_ref[v].T
        total = jnp.zeros((HX, TAB), F32)
        for i in range(12):
            piece = turned[HX * i : HX * i + HX, :].astype(BF16)
            total = total + nn(piece, sel_ref[ROWS * i : ROWS * i + ROWS, :])
        for t in range(3):
            tab_ref[ROWS * t + HX * v : ROWS * t + HX * v + HX, :] = total[:, 128 * t : 128 * t + 128]
    tab_ref[3 * ROWS :, :] = jnp.zeros((16 * SLOT - 3 * ROWS, 128), F32)
    low_ref[...] = tab_ref[...].astype(BF16)
    for k, group in enumerate((grad_q, grad_k, grad_v)):
        for g in range(4):
            few_ref[k, ROWS * g : ROWS * g + ROWS, :] = group[g]
    few_ref[3] = normed
    few_ref[4] = normed2
    few_ref[5] = cot_low
    few_ref[6] = attn_grad
    few_ref[7] = attended
    wide_ref[0] = pre_grad
    wide_ref[1] = activated
    hat_ref[...] = hat1
    inv_ref[...] = inv1
    rg_ref[...] = resid_grad
    row_ref[0:1, :] = pb_sum
    row_ref[1:2, :] = f2_sum
    row_ref[2:3, :] = n2g_sum
    row_ref[3:4, :] = n2o_sum
    f1s_ref[...] = f1_sum


def back_kernel(core_ref, n1g_ref, few_ref, wide_ref, hat_ref, inv_ref, rg_ref, row_ref,
                f1s_ref, wt_ref, ra_ref, ca_ref, rb_ref, cb_ref,
                ig_ref, own_ref, send_ref, stage_ref):
    wq = wt_ref[0:192, :]
    wk = wt_ref[192:384, :]
    wv = wt_ref[384:576, :]
    n1g = n1g_ref[...].reshape(1, -1)
    dq = few_ref[0]
    dk = few_ref[1]
    dv = few_ref[2]
    normed = few_ref[3]
    hat1 = hat_ref[...]
    f1_sum = f1s_ref[...]
    pb_sum = row_ref[0:1, :]
    f2_sum = row_ref[1:2, :]
    n2g_sum = row_ref[2:3, :]
    n2o_sum = row_ref[3:4, :]
    n1_grad = nn(dq, wq) + nn(dk, wk) + nn(dv, wv)
    n1g_sum = jnp.sum(n1_grad * hat1, axis=0, keepdims=True)
    n1o_sum = jnp.sum(n1_grad, axis=0, keepdims=True)
    input_grad = (rg_ref[...] + norm_back(n1_grad, hat1, inv_ref[...], n1g)).astype(BF16)
    ig_ref[...] = input_grad
    sums = [jnp.sum(d.astype(F32), axis=0, keepdims=True) for d in (dq, dk, dv)]
    dw_q = tn(dq, normed)
    dw_k = tn(dk, normed)
    dw_v = tn(dv, normed)
    dw_qkv = jnp.concatenate([dw_q, dw_k, dw_v], axis=0)
    dw_p = tn(few_ref[6], few_ref[7])
    dw_1 = tn(wide_ref[0], few_ref[4])
    dw_2 = tn(few_ref[5], wide_ref[1])
    vec_a = jnp.concatenate(sums + [f1_sum[:, 0:192], f1_sum[:, 192:384], f1_sum[:, 384:576], f1_sum[:, 576:768]], axis=1)
    vec_b = jnp.concatenate([pb_sum, f2_sum, n1g_sum, n1o_sum, n2g_sum, n2o_sum], axis=1)
    row_a = nn((ra_ref[...].astype(F32) * vec_a).astype(BF16), ca_ref[...])
    row_b = nn((rb_ref[...].astype(F32) * vec_b).astype(BF16), cb_ref[...])
    for l in range(16):
        a36 = dw_qkv[36 * l : 36 * l + 36]
        a12 = dw_p[12 * l : 12 * l + 12]
        b48 = dw_1[48 * l : 48 * l + 48]
        d12 = dw_2[12 * l : 12 * l + 12]
        top = PART * l
        stage_ref[0, top : top + 36, :] = a36[:, :128]
        stage_ref[0, top + 36 : top + 48, :] = a12[:, :128]
        a_rest = jnp.concatenate([a36[:, 128:], a12[:, 128:]], axis=0)
        stage_ref[0, top + 48 : top + 96, :] = jnp.concatenate([a_rest, b48[:, 128:]], axis=1)
        stage_ref[0, top + 96 : top + 108, :] = d12[:, 640:]
        stage_ref[0, top + 108 : top + 109, :] = row_a[l : l + 1]
        stage_ref[0, top + 109 : top + 110, :] = row_b[l : l + 1]
        stage_ref[0, top + 110 : top + 112, :] = jnp.zeros((2, 128), F32)
        stage_ref[1, top : top + 48, :] = b48[:, :128]
        for b in range(5):
            stage_ref[1, top + 48 + 12 * b : top + 60 + 12 * b, :] = d12[:, 128 * b : 128 * b + 128]
        stage_ref[1, top + 108 : top + 112, :] = jnp.zeros((4, 128), F32)
    core = core_ref[0]
    own_ref[...] = stage_ref[core].astype(BF16)
    send_ref[...] = stage_ref[1 - core].astype(BF16)


def place_kernel(block_ref, ig_ref, back_ref, out_ref, edge_ref):
    back = back_ref[...]
    for k, ref in enumerate((block_ref, ig_ref)):
        placed = nn(back, ref[...]).astype(BF16)
        out_ref[k] = placed[:576]
        edge_ref[k] = placed[576:]


def edge_kernel(x_hbm, cot_hbm, out_ref, sems):
    copies = [
        pltpu.make_async_copy(src.at[:, 0:8, :], out_ref.at[k], sems.at[k])
        for k, src in enumerate((x_hbm, cot_hbm))
    ]
    for copy in copies:
        copy.start()
    for copy in copies:
        copy.wait()


def join_kernel(own_ref, got_ref, tab_ref, out_ref):
    for l in range(16):
        part = slice(PART * l, PART * l + PART)
        out_ref[l, 0:PART, :] = (own_ref[part].astype(F32) + got_ref[part].astype(F32)).astype(BF16)
        out_ref[l, PART:, :] = tab_ref[SLOT * l : SLOT * l + SLOT]


def lon_sum_kernel(in_ref, out_ref):
    total = in_ref[0].astype(F32)
    for l in range(1, 16):
        total = total + in_ref[l].astype(F32)
    low = total.astype(BF16)
    for k in range(8):
        out_ref[k] = low


def band_sum_kernel(y_ref, in_ref, out_ref, tab_ref):
    total = in_ref[0, 0:PART].astype(F32)
    for k in range(1, 8):
        total = total + in_ref[k, 0:PART].astype(F32)
    out_ref[...] = total.astype(BF16)
    y = y_ref[0]
    low = (in_ref[2 * y, PART:].astype(F32) + in_ref[2 * y + 1, PART:].astype(F32)).astype(BF16)
    for l in range(16):
        tab_ref[l] = low


def weight_kernel(core_ref, own_ref, got_ref, qw_ref, pw_ref, f1_ref, f2_ref, qb_ref, pb_ref, f1b_ref,
                  f2b_ref, n1g_ref, n1o_ref, n2g_ref, n2o_ref, pair_ref):
    core = core_ref[0]
    pair_ref[core] = own_ref[...].astype(F32) * FACTOR
    pair_ref[1 - core] = got_ref[...].astype(F32) * FACTOR
    first = pair_ref[0]
    second = pair_ref[1]
    a = jnp.concatenate([first[0:48], first[48:96, 0:64]], axis=1)
    qw_ref[...] = a[0:36]
    pw_ref[...] = a[36:48]
    f1_ref[...] = jnp.concatenate([second[0:48], first[48:96, 64:128]], axis=1)
    d = [second[48 + 12 * k : 60 + 12 * k] for k in range(5)] + [first[96:108]]
    f2_ref[...] = jnp.concatenate(d, axis=1)
    va = first[108:109]
    vb = first[109:110]
    qb_ref[...] = va[:, 0:36].reshape(36)
    f1b_ref[...] = va[:, 36:84].reshape(48)
    for k, ref in enumerate((pb_ref, f2b_ref, n1g_ref, n1o_ref, n2g_ref, n2o_ref)):
        ref[...] = vb[:, 12 * k : 12 * k + 12].reshape(12)


def table_kernel(tab_ref, out_tab_ref):
    tab = tab_ref[...].astype(F32)
    for t in range(3):
        tile = tab[ROWS * t : ROWS * t + ROWS]
        for k in range(4):
            piece = pltpu.roll(tile, 128 - 32 * k, 1) if k else tile
            out_tab_ref[pl.ds(4 * t + k, ROWS, stride=12), :] = piece[:, :23]


def call(kernel, out_shape, smem=0, far=0, near=0, limit=8, scratch=(), raw=False, flops=0):
    count = smem + far + near
    space = pltpu.HBM if raw else pltpu.VMEM
    specs = [pl.BlockSpec(memory_space=pltpu.SMEM)] * smem + [
        pl.BlockSpec(memory_space=space)
    ] * (far + near)
    run = pl.pallas_call(
        kernel,
        out_shape=out_shape,
        in_specs=specs,
        out_specs=jax.tree.map(lambda _: pl.BlockSpec(memory_space=pltpu.VMEM), out_shape),
        scratch_shapes=scratch,
        compiler_params=pltpu.CompilerParams(vmem_limit_bytes=limit << 20),
        cost_estimate=pl.CostEstimate(flops=flops, transcendentals=0, bytes_accessed=0)
        if flops
        else None,
    )

    def go(*args):
        if raw:
            args = tuple(pltpu.with_memory_space_constraint(a, pltpu.HBM) for a in args)
        kept = args[: smem + far] + tuple(
            pltpu.with_memory_space_constraint(a, pltpu.VMEM) for a in args[smem + far :]
        )
        assert len(args) == count
        return run(*kept)

    return go


def near(dims, dtype):
    return pltpu.VMEM(dims, dtype)


def shape(dims, dtype):
    return jax.ShapeDtypeStruct(dims, dtype)


def on_device(inputs, cotangent, norm1_gain, norm1_offset, qkv_weight, qkv_bias, bias_table,
              proj_weight, proj_bias, norm2_gain, norm2_offset, fc1_weight, fc1_bias,
              fc2_weight, fc2_bias):
    grid = inputs.shape
    x = inputs.reshape(576, C)
    cot = cotangent.reshape(576, C)
    edge = call(
        edge_kernel, near((2, 24, 8, C), BF16), far=2, raw=True,
        scratch=[pltpu.SemaphoreType.DMA((2,))],
    )(inputs.reshape(24, 24, C), cotangent.reshape(24, 24, C)).reshape(2, 192, C)
    halo = lax.ppermute(edge, "lon", [(k, (k - 1) % 16) for k in range(16)])
    table = bias_table.reshape(12 * ROWS, 23)
    wt, proj, fc1, fc2, bias, spread, mask, sel, ra, ca, rb, cb, picks, back = call(
        prep_kernel,
        [near((576, C), BF16), near((C, C), BF16), near((C, FF), BF16), near((C, FF), BF16),
         near((2, ROWS, LANES), F32), near((ROWS, LANES), BF16), near((C, LANES), BF16),
         near((12 * ROWS, TAB), BF16), near((16, 1344), BF16), near((1344, 128), BF16),
         near((16, 1152), BF16), near((1152, 128), BF16), near((576, 768), BF16), near((768, 576), BF16)],
        far=5,
        limit=16,
        raw=True,
        scratch=[pltpu.VMEM((C, 576), F32), pltpu.VMEM((C, C), F32), pltpu.VMEM((C, FF), F32),
                 pltpu.VMEM((C, FF), F32), pltpu.VMEM((12 * ROWS, 23), F32),
                 pltpu.SemaphoreType.DMA((5,))],
    )(qkv_weight, proj_weight, fc1_weight, fc2_weight.T, table)
    core = lax.axis_index("core").astype(jnp.int32).reshape(1)
    tab, block, *state = call(
        front_kernel,
        [near((16 * SLOT, 128), BF16), near((576, C), BF16), near((8, 576, C), BF16),
         near((2, 576, FF), BF16), near((576, C), F32), near((576, 1), F32), near((576, C), F32),
         near((8, C), F32), near((1, FF), F32)],
        far=10,
        near=10,
        limit=24,
        scratch=[pltpu.VMEM((2, ROWS, LANES), F32), pltpu.VMEM((16 * SLOT, 128), F32)],
    )(x, cot, norm1_gain, norm1_offset, qkv_bias, proj_bias, norm2_gain, norm2_offset, fc1_bias,
      fc2_bias, halo, bias, wt, proj, fc1, fc2, spread, mask, sel, picks)
    slope, own, send = call(
        back_kernel,
        [near((576, C), BF16), near((16 * PART, 128), BF16), near((16 * PART, 128), BF16)],
        smem=1,
        far=1,
        near=12,
        limit=16,
        scratch=[pltpu.VMEM((2, 16 * PART, 128), F32)],
    )(core, norm1_gain, *state, wt, ra, ca, rb, cb)
    got = lax.ppermute(send, "core", [(0, 1), (1, 0)])
    joined = call(join_kernel, near((16, PART + SLOT, 128), BF16), near=3)(own, got, tab)
    arrived = lax.all_to_all(joined, "lon", split_axis=0, concat_axis=0, tiled=True)
    both, ends = call(
        place_kernel, [near((2, 576, C), BF16), near((2, 192, C), BF16)], near=3
    )(block, slope, back)
    home = lax.ppermute(ends, "lon", [(k, (k + 1) % 16) for k in range(16)])
    copies = call(lon_sum_kernel, near((8, PART + SLOT, 128), BF16), near=1)(arrived)
    bands = lax.all_to_all(copies, ("y", "ens"), split_axis=0, concat_axis=0, tiled=True)
    band = lax.axis_index("y").astype(jnp.int32).reshape(1)
    half, tab_copies = call(
        band_sum_kernel, [near((PART, 128), BF16), near((16, SLOT, 128), BF16)], smem=1, near=1
    )(band, bands)
    tab_all = lax.all_to_all(tab_copies, "lon", split_axis=0, concat_axis=0, tiled=True)
    other = lax.ppermute(half, "core", [(0, 1), (1, 0)])
    qw, pw, f1, f2, qb, pb, f1b, f2b, n1g, n1o, n2g, n2o = call(
        weight_kernel,
        [shape((36, C), F32), shape((12, C), F32), shape((48, C), F32), shape((12, FF), F32),
         shape((36,), F32), shape((12,), F32), shape((48,), F32)] + [shape((12,), F32)] * 5,
        smem=1,
        near=2,
        scratch=[pltpu.VMEM((2, PART, 128), F32)],
    )(core, half, other)
    tab_out = call(table_kernel, shape((12 * ROWS, 23), F32), near=1)(
        tab_all.reshape(16 * SLOT, 128)
    )
    full = both.reshape(2, *grid[1:])
    ends = home.reshape(2, grid[1], grid[2], 8, C)[:, :, :, :6]
    full = jnp.concatenate([ends, full[:, :, :, 6:]], axis=3)
    return (full[0][None], full[1][None], qw.T, qb, pw.T, pb, f1.T, f1b, f2.T, f2b, n1g, n1o, n2g, n2o,
            tab_out.reshape(bias_table.shape))


def solution(mesh):
    split = Mesh(mesh.devices.reshape(16, 4, 2, 2), ("lon", "y", "core", "ens"))
    lat = ("y", "core")
    tokens = P("ens", None, lat, "lon", None)
    table = P(None, lat, None, None, None, None)
    return jax.shard_map(
        on_device,
        mesh=split,
        in_specs=(tokens, tokens, P(), P(), P(), P(), table) + (P(),) * 8,
        out_specs=(tokens, tokens, P(None, "lon"), P("lon"), P(None, "lon"), P("lon"), P(None, "lon"),
                   P("lon"), P(None, "lon"), P("lon"), P("lon"), P("lon"), P("lon"), P("lon"), table),
        check_vma=False,
    )
```
